32 devices in a mesh: district: 4 (over y, core), sub: 8 (over z, x).
Axes of the slice: x: 2, y: 2, z: 4, core: 2. Of those that a mesh axis runs over, the one named last changes fastest.
Arguments:
- cost_terms: bfloat16 [8, 512, 768], P('district', 'sub'), may hold values from -6 to 6
- neighbours: int32 [8, 512, 4], P('district', 'sub'), may hold values from 0 to 511, as said below
- relayout: int32 [8, 512], P('district'), may hold values from 0 to 511, as said below
- ownership: int32 [8, 512], P('district', 'sub'), may hold values from 0 to 31
- capacity: float32 [16, 48], replicated, may hold values from -67.88225 to 67.88225
- coupling: bfloat16 [8, 768, 192], P('district'), may hold values from -0.21875 to 0.21875
- solve_factor: bfloat16 [8, 768, 768], P('district')
Outputs:
- control_plan: float32 [8, 512, 768], P('district', 'sub')
- flow_prices: float32 [8, 512, 192], P('district', 'sub')
- reservoir_duals: float32 [16, 48], replicated
The draws below stay inside these ranges and needn't reach their ends.
Inputs may be any that keep to these rules, and one draw needn't show every extreme that they name: `neighbours`: each entry lies within 16 of its own balanced position and differs from it. `relayout`: each row is a permutation; of the subsystems at geographic positions s * 64 to (s + 1) * 64 - 1, exactly 8 go to balanced positions j * 64 to (j + 1) * 64 - 1, for every s and j. `ownership`: values of 16 or more mean that the subsystem draws from no reservoir.
All inputs are finite; a program needn't handle non-finite values.
Results may differ from the reference program's by a relative error of at most 0.018.
Values may be sent and summed in bfloat16 or wider, within the bound.
A program may use at most 64 MiB of HBM per device.

```python
import math
import jax
import jax.numpy as jnp
from jax import lax

HORIZON = 48
UNKNOWNS = 768
INTERFACE = 192
SUB_DEV = 64
DISTRICTS = 8
SUB_DIST = 512
PEER_SHARE = 8
REACH_SPAN = 16
LINK_COUNT = 4
RESERVOIRS = 16
RESERVOIR_LOAD = 128
OUTER_ITERS = 2
INNER_ITERS = 4


def draw_neighbours(key, part):
    picks = jax.random.randint(key, (DISTRICTS, SUB_DIST, LINK_COUNT), 0, 2 * REACH_SPAN)
    offsets = picks - REACH_SPAN + (picks >= REACH_SPAN).astype(jnp.int32)
    places = jnp.arange(SUB_DIST, dtype=jnp.int32)[None, :, None]
    target = places + offsets
    target = jnp.where((target < 0) | (target >= SUB_DIST), places - offsets, target)
    return target.astype(jnp.int32)


def draw_relayout(key, part):
    first_key = jax.random.fold_in(key, 11)
    second_key = jax.random.fold_in(key, 23)
    groups = SUB_DIST // SUB_DEV
    base = jnp.tile(jnp.arange(SUB_DEV, dtype=jnp.int32)[None, :], (DISTRICTS * groups, 1))
    source_perm = jax.random.permutation(first_key, base, axis=1, independent=True).reshape(DISTRICTS, groups, SUB_DEV)
    target_perm = jax.random.permutation(second_key, base, axis=1, independent=True).reshape(DISTRICTS, groups, SUB_DEV)
    dest_block = source_perm // PEER_SHARE
    within = source_perm % PEER_SHARE
    sources = jnp.arange(groups, dtype=jnp.int32)[None, :, None]
    slot_index = sources * PEER_SHARE + within
    district_rows = jnp.arange(DISTRICTS, dtype=jnp.int32)[:, None, None]
    target = dest_block * SUB_DEV + target_perm[district_rows, dest_block, slot_index]
    return target.reshape(DISTRICTS, SUB_DIST).astype(jnp.int32)


def draw_solve_factor(key, part):
    first_key = jax.random.fold_in(key, 5)
    second_key = jax.random.fold_in(key, 7)
    diagonal = jnp.exp(jax.random.uniform(first_key, (DISTRICTS, UNKNOWNS), jnp.float32, jnp.log(0.5), jnp.log(2.0)))
    spread = jax.random.normal(second_key, (DISTRICTS, UNKNOWNS, UNKNOWNS), jnp.float32) * (0.5 / UNKNOWNS ** 0.5)
    matrix = spread + diagonal[:, :, None] * jnp.eye(UNKNOWNS, dtype=jnp.float32)[None, :, :]
    return matrix.astype(jnp.bfloat16)


def set_ends(entries, own_key, low, high):
    dims = entries.shape
    index_at = [jax.random.randint(jax.random.fold_in(own_key, axis), (), 0, dims[axis]) for axis in range(len(dims))]
    entries = entries.at[tuple(index_at)].set(low)
    longest = dims.index(max(dims))
    index_at[longest] = (index_at[longest] + 1) % dims[longest]
    return entries.at[tuple(index_at)].set(high)


def shard_levels(key, shape, pieces, least, high):
    factor_of, own = 1.0, jax.random.fold_in(key, 6)
    for position, parts in pieces:
        heights = jnp.exp(jax.random.uniform(jax.random.fold_in(own, position), (parts,), jnp.float32, least / len(pieces), high / len(pieces)))
        factor_of = factor_of * jnp.repeat(heights, shape[position] // parts).reshape([-1 if axis == position else 1 for axis in range(len(shape))])
    return factor_of


def normal_values(stream_key, shape, scale, limit, split=(), held_as=jnp.bfloat16):
    values = scale * jax.random.normal(stream_key, shape, jnp.float32)
    if split:
        values = values * shard_levels(stream_key, shape, split, -0.22, 0.18)
    return jnp.clip(values, -limit, limit).astype(held_as)


def setup_inputs(seed: int = 0) -> dict:
    seeds = jax.random.split(jax.random.key(seed), 8)
    return {
        "cost_terms": normal_values(seeds[0], (DISTRICTS, SUB_DIST, UNKNOWNS), 1.0, 6.0, ((0, 4), (1, 8))),
        "neighbours": draw_neighbours(jax.random.fold_in(seeds[7], 71), 0),
        "relayout": draw_relayout(jax.random.fold_in(seeds[7], 71), 0),
        "ownership": set_ends(jax.random.randint(seeds[3], (DISTRICTS, SUB_DIST), 0, 2 * RESERVOIRS), jax.random.fold_in(seeds[3], 1), 0, (2 * RESERVOIRS) - 1).astype(jnp.int32),
        "capacity": normal_values(seeds[4], (RESERVOIRS, HORIZON), (RESERVOIR_LOAD ** 0.5), 67.88225, (), jnp.float32),
        "coupling": normal_values(seeds[5], (DISTRICTS, UNKNOWNS, INTERFACE), UNKNOWNS ** -0.5, 0.21875, ((0, 4),)),
        "solve_factor": draw_solve_factor(jax.random.fold_in(seeds[7], 71), 0),
    }


price_step = 0.3
reserve_step = 1.0

def neighbour_mean(values, links):
    district_rows = jnp.arange(values.shape[0], dtype=jnp.int32)[:, None]
    running = jnp.zeros(links.shape[:2] + values.shape[2:], jnp.float32)
    for which in range(LINK_COUNT):
        running = running + values[district_rows, links[:, :, which]].astype(jnp.float32)
    return running / LINK_COUNT

def reference(cost_terms, neighbours, relayout, ownership, capacity, coupling, solve_factor):
    district_rows = jnp.arange(DISTRICTS, dtype=jnp.int32)[:, None]
    inverse = jnp.argsort(relayout, axis=1, stable=True).astype(jnp.int32)
    balanced_costs = cost_terms[district_rows, inverse]
    owner_slot = jnp.where(ownership < RESERVOIRS, ownership, RESERVOIRS).astype(jnp.int32)
    flow_prices = jnp.zeros((DISTRICTS, SUB_DIST, INTERFACE), jnp.float32)
    reserve_duals = jnp.zeros((RESERVOIRS, HORIZON), jnp.float32)
    dual_scale = reserve_step / math.sqrt(RESERVOIR_LOAD)
    highest = lax.Precision.HIGHEST
    coupling_wide = coupling.astype(jnp.float32)
    factor_wide = solve_factor.astype(jnp.float32)
    plan_now = None
    flow_now = None
    for outer_step in range(OUTER_ITERS):
        for inner_step in range(INNER_ITERS):
            padded_duals = jnp.concatenate([reserve_duals, jnp.zeros((1, HORIZON), jnp.float32)], axis=0)
            boundary = padded_duals[owner_slot]
            boundary = jnp.concatenate([boundary, jnp.zeros((DISTRICTS, SUB_DIST, INTERFACE - HORIZON), jnp.float32)], axis=2)
            price_term = (flow_prices - neighbour_mean(flow_prices, neighbours) + boundary).astype(jnp.bfloat16)
            gradient = (balanced_costs.astype(jnp.float32) + jnp.einsum('dsf,dzf->dsz', price_term.astype(jnp.float32), coupling_wide, precision=highest)).astype(jnp.bfloat16)
            plan_now = -jnp.einsum('dsz,dzw->dsw', gradient.astype(jnp.float32), factor_wide, precision=highest)
            plan_rounded = plan_now.astype(jnp.bfloat16)
            flow_now = jnp.einsum('dsz,dzf->dsf', plan_rounded.astype(jnp.float32), coupling_wide, precision=highest).astype(jnp.bfloat16)
            flow_prices = flow_prices + price_step * (flow_now.astype(jnp.float32) - neighbour_mean(flow_now, neighbours))
        draws = jax.ops.segment_sum(flow_now[:, :, :HORIZON].astype(jnp.float32).reshape(-1, HORIZON), owner_slot.reshape(-1), num_segments=RESERVOIRS + 1)[:RESERVOIRS]
        reserve_duals = reserve_duals + (draws - capacity) * dual_scale
    control_plan = plan_now[district_rows, relayout]
    return (control_plan, flow_prices, reserve_duals)
```

```python
import functools
import math

import jax
import jax.numpy as jnp
from jax import lax
from jax.experimental import pallas as pl
from jax.experimental.pallas import tpu as pltpu
from jax.sharding import PartitionSpec as P

REACH_SPAN = 16
LINK_COUNT = 4
RESERVOIRS = 16
OUTER_ITERS = 2
INNER_ITERS = 4
HALO = 2 * REACH_SPAN
LANES = 128

price_step = 0.3
reserve_step = 1.0

F32 = jnp.float32
BF16 = jnp.bfloat16
MESH = pl.DeviceIdType.MESH


def each(count, body):
    if count <= 8:
        for index in range(count):
            body(index)
    else:
        lax.fori_loop(0, count, lambda index, carry: (body(index), carry)[1], 0)


def mm(a, b):
    return jnp.dot(a, b, preferred_element_type=F32)


def contract(a, b, dim):
    return lax.dot_general(a, b, (((dim,), (dim,)), ((), ())), preferred_element_type=F32)


def fold(wide, half):
    tail = wide[:, LANES:]
    lane = lax.broadcasted_iota(jnp.int32, (half, LANES), 1)
    folded = jnp.where(lane < LANES // 2, tail[:half], pltpu.roll(tail[half:], LANES // 2, 1))
    return jnp.concatenate([wide[:, :LANES], folded], axis=0)


def unfold(folded, rows):
    tail = folded[rows:]
    return jnp.concatenate([tail, pltpu.roll(tail, LANES // 2, 1)], axis=0)


def target_of(index, me, count):
    low = 1 - jnp.minimum(me // (count // 2), 1)
    climb = index + jnp.minimum(jnp.maximum(index - me + 1, 0), 1)
    fall = count - 1 - index
    fall = fall - jnp.minimum(jnp.maximum(me - fall + 1, 0), 1)
    return low * fall + (1 - low) * climb


def kernel(
    dual_scale, costs_hbm, near_hbm, owner_hbm, relayout_hbm, capacity_hbm, coupling_hbm, factor_hbm,
    plan_ref, prices_ref, duals_ref,
    costs_ref, near_ref, owner_ref, relayout_ref, capacity_ref, coupling, factor, tables, near, links, owners, wide_first, first, landed, gathered, base, state, flow, total, spread, weight,
    match, match_t, select, near_links, chosen_out, chosen_in, prices_out, prices_in, duals, draws, arrived,
    local_sem, near_send, near_recv, flow_send, flow_recv, draw_send, draw_recv,
    price_send, price_recv, dual_send, dual_recv,
):
    districts, rows, unknowns = costs_ref.shape
    interface = coupling.shape[1]
    horizon = capacity_ref.shape[1]
    group = relayout_ref.shape[1]
    sub_count = lax.axis_size("sub")
    district_count = lax.axis_size("district")
    me = lax.axis_index("sub")
    role = lax.rem(me, districts)
    team = me // districts * districts
    my_district = lax.axis_index("district")
    block = districts * rows
    window = block + 2 * HALO
    blocks = group // block

    costs_load = pltpu.make_async_copy(costs_hbm, costs_ref, local_sem.at[2 * districts])
    costs_load.start()
    loads = []
    for d in range(districts):
        loads.append(
            (
                pltpu.make_async_copy(factor_hbm.at[d], factor.at[d], local_sem.at[2 * d]),
                pltpu.make_async_copy(coupling_hbm.at[d], coupling.at[d], local_sem.at[2 * d + 1]),
            )
        )
        for load in loads[-1]:
            load.start()

    small_loads = [
        pltpu.make_async_copy(source, target, local_sem.at[2 * districts + 1 + index])
        for index, (source, target) in enumerate(
            (
                (near_hbm, near_ref),
                (owner_hbm, owner_ref),
                (relayout_hbm, relayout_ref),
                (capacity_hbm, capacity_ref),
            )
        )
    ]
    for load in small_loads:
        load.start()

    barrier = pltpu.get_barrier_semaphore()
    for step in range(1, sub_count):
        pl.semaphore_signal(
            barrier, inc=1, device_id={"sub": lax.rem(me + step, sub_count)}, device_id_type=MESH
        )
    for step in range(1, district_count):
        for other in range(districts):
            pl.semaphore_signal(
                barrier,
                inc=1,
                device_id={
                    "district": lax.rem(my_district + step, district_count),
                    "sub": team + lax.rem(role + other, districts),
                },
                device_id_type=MESH,
            )

    costs_load.wait()
    for d in range(districts):
        for load in loads[d]:
            load.wait()
        first_plan = -mm(costs_ref[d], factor[d])
        wide_first[:, :interface] = contract(first_plan.astype(BF16), coupling[d], 1)
        first[d] = fold(wide_first[...], rows // 2).astype(BF16)

    for load in small_loads:
        load.wait()
    for d in range(districts):
        for k in range(LINK_COUNT):
            tables[d, k // 2 : k // 2 + 1, k % 2 * rows : (k % 2 + 1) * rows] = near_ref[d * LINK_COUNT + k : d * LINK_COUNT + k + 1, :]
        tables[d, LINK_COUNT // 2 : LINK_COUNT // 2 + 1, :rows] = owner_ref[d : d + 1, :]
    pl.semaphore_wait(barrier, sub_count - 1 + (district_count - 1) * districts)
    sends = []
    for index in range(sub_count - 1):
        target = target_of(index, me, sub_count)
        sends.append(
            pltpu.make_async_remote_copy(
                src_ref=tables.at[lax.rem(target, districts)],
                dst_ref=near.at[me],
                send_sem=near_send.at[index],
                recv_sem=near_recv.at[me],
                device_id={"sub": target},
                device_id_type=MESH,
            )
        )
        sends[-1].start()
    for index in range(sub_count - 1):
        target = target_of(index, me, sub_count)
        sends.append(
            pltpu.make_async_remote_copy(
                src_ref=first.at[lax.rem(target, districts)],
                dst_ref=landed.at[me],
                send_sem=flow_send.at[index],
                recv_sem=flow_recv.at[me],
                device_id={"sub": target},
                device_id_type=MESH,
            )
        )
        sends[-1].start()

    landed[me] = first[role]
    narrow = mm(coupling[role], factor[role]).astype(BF16)
    weight[...] = (-contract(narrow, coupling[role], 1)).astype(BF16)

    wide = rows + 2 * HALO
    moves = relayout_ref[pl.ds(role, 1), :]
    team_rows = districts * rows
    pick = lax.broadcasted_iota(jnp.int32, (team_rows, group), 1) == (
        lax.broadcasted_iota(jnp.int32, (team_rows, group), 0) + team * rows
    )
    pick = jnp.where(pick, 1.0, 0.0).astype(BF16)

    def choose(b):
        place = lax.broadcasted_iota(jnp.int32, (block, group), 0) + b * block
        chosen = jnp.where(place == moves, 1.0, 0.0).astype(BF16)
        select[b] = contract(pick, chosen, 1).astype(BF16)

    each(blocks, choose)

    duals[...] = jnp.zeros_like(duals)
    duals[:, :horizon] = capacity_ref[...]
    capacity = duals[...]
    flow[...] = jnp.zeros_like(flow)
    links[...] = jnp.full_like(links, -window * 4)

    near[me] = tables[role]
    for step in range(1, sub_count):
        source = lax.rem(me + step, sub_count)
        pltpu.make_async_remote_copy(
            src_ref=tables.at[role],
            dst_ref=near.at[source],
            send_sem=near_send.at[step - 1],
            recv_sem=near_recv.at[source],
            device_id={"sub": source},
            device_id_type=MESH,
        ).wait_recv()
    for source in range(sub_count):
        for k in range(LINK_COUNT):
            links[k : k + 1, HALO + source * rows : HALO + (source + 1) * rows] = near[source, k // 2 : k // 2 + 1, k % 2 * rows : (k % 2 + 1) * rows]
        owners[:, source * rows : (source + 1) * rows] = near[source, LINK_COUNT // 2 : LINK_COUNT // 2 + 1, :rows]
    own = owners[...]
    hit = jnp.where(
        lax.broadcasted_iota(jnp.int32, (RESERVOIRS, group), 0) == own, 1.0, 0.0
    ).astype(F32)
    match_t[...] = hit.astype(BF16)
    match[...] = hit.T.astype(BF16)

    def linked(start, width):
        column = lax.broadcasted_iota(jnp.int32, (width, width), 0)
        row = lax.broadcasted_iota(jnp.int32, (width, width), 1)
        table = jnp.where(column == row, 1.0, 0.0)
        for k in range(LINK_COUNT):
            link = links[k : k + 1, pl.ds(start, width)] - (start - HALO)
            table = table - jnp.where(column == link, 1.0 / LINK_COUNT, 0.0)
        return table.T.astype(BF16)

    def build(b):
        start = b * block if isinstance(b, int) else pl.multiple_of(b * block, block)
        table = linked(start, window)
        spread[b] = mm(table[HALO : HALO + block], table).astype(BF16)

    each(blocks, build)
    near_links[...] = linked(pl.multiple_of(team * rows, team_rows), window)[HALO : HALO + team_rows]

    for step in range(1, sub_count):
        source = lax.rem(me + step, sub_count)
        pltpu.make_async_remote_copy(
            src_ref=first.at[role],
            dst_ref=landed.at[source],
            send_sem=flow_send.at[step - 1],
            recv_sem=flow_recv.at[source],
            device_id={"sub": source},
            device_id_type=MESH,
        ).wait_recv()

    def spread_out(source):
        at = pl.ds(source * rows, rows)
        gathered[at, :LANES] = landed[source, :rows, :]
        gathered[at, LANES:] = unfold(landed[source].astype(F32), rows).astype(BF16)

    each(sub_count, spread_out)

    def at_block(b, extra=0, size=block):
        return pl.ds(b * block + extra, size)

    def permute(b):
        place = lax.broadcasted_iota(jnp.int32, (block, group), 0) + b * block
        chosen = jnp.where(place == moves, 1.0, 0.0).astype(BF16)
        moved = mm(chosen, gathered[...])[:, :interface]
        base[at_block(b), :] = moved
        flow[at_block(b, HALO), :] = moved.astype(BF16)

    each(blocks, permute)

    team_window = pl.ds(pl.multiple_of(team * rows, team_rows), window)
    total[...] = flow[team_window, :].astype(F32)

    def begin(b):
        state[at_block(b), :] = price_step * mm(spread[b], flow[at_block(b, 0, window), :])

    each(blocks, begin)

    def forward():
        def one(b):
            price = state[at_block(b), :].astype(BF16)
            flow[at_block(b, HALO), :] = (base[at_block(b), :] + mm(price, weight[...])).astype(BF16)

        each(blocks, one)
        total[...] += flow[team_window, :].astype(F32)

    def backward():
        def one(b):
            state[at_block(b), :] += price_step * mm(spread[b], flow[at_block(b, 0, window), :])

        each(blocks, one)

    def inner(step, carry):
        forward()
        backward()
        return carry

    partners = [
        (step, other)
        for step in range(district_count)
        for other in range(districts)
        if step or other
    ]

    def partner(step, other):
        return {
            "district": lax.rem(my_district + step, district_count),
            "sub": team + lax.rem(role + other, districts),
        }

    def send_draws(outer):
        drawn = mm(match_t[...], flow[HALO : HALO + group, :])
        draws[outer] = drawn[:, :LANES]
        copies = []
        for index, (step, other) in enumerate(partners):
            copies.append(
                pltpu.make_async_remote_copy(
                    src_ref=draws.at[outer],
                    dst_ref=arrived.at[outer, index],
                    send_sem=draw_send.at[outer, index],
                    recv_sem=draw_recv.at[outer, index],
                    device_id=partner(step, other),
                    device_id_type=MESH,
                )
            )
            copies[-1].start()
        return copies

    def take_draws(outer, copies):
        drawn = draws[outer]
        for index, copy in enumerate(copies):
            copy.wait()
            drawn = drawn + arrived[outer, index]
        lane = lax.broadcasted_iota(jnp.int32, drawn.shape, 1)
        return jnp.where(lane < horizon, (drawn - capacity) * dual_scale, 0.0)

    def to_team(source_ref, place_ref, send_sem, recv_sem):
        copies = []
        for other in range(1, districts):
            target = lax.rem(role + other, districts)
            copies.append(
                pltpu.make_async_remote_copy(
                    src_ref=source_ref.at[target],
                    dst_ref=place_ref.at[role],
                    send_sem=send_sem.at[other],
                    recv_sem=recv_sem.at[other],
                    device_id={"sub": team + target},
                    device_id_type=MESH,
                )
            )
            copies[-1].start()
        return copies

    lax.fori_loop(1, INNER_ITERS - 1, inner, 0)
    forward()
    copies = send_draws(0)
    backward()
    moved = take_draws(0, copies)
    for outer in range(1, OUTER_ITERS):
        duals[...] = moved if outer == 1 else duals[...] + moved
        high = moved.astype(BF16)
        low = (moved - high.astype(F32)).astype(BF16)
        state[:, :LANES] += mm(match[...], high) + mm(match[...], low)
        lax.fori_loop(0, INNER_ITERS - 1, inner, 0)
        if outer == OUTER_ITERS - 1:
            price = state[...].astype(BF16)
            chosen = mm(select[0], price[:block])
            for b in range(1, blocks):
                chosen = chosen + mm(select[b], price[b * block : (b + 1) * block])
            chosen_out[...] = chosen.reshape(districts, rows, -1).astype(BF16)
            price_copies = to_team(chosen_out, chosen_in, price_send, price_recv)
            chosen_in[role] = chosen_out[role]
        forward()
        copies = send_draws(outer)
        if outer < OUTER_ITERS - 1:
            backward()
        else:
            high = total[...].astype(BF16)
            low = (total[...] - high.astype(F32)).astype(BF16)
            prices = price_step * (mm(near_links[...], high) + mm(near_links[...], low))
            prices_out[...] = prices.reshape(districts, rows, -1)
            dual_copies = to_team(prices_out, prices_in, dual_send, dual_recv)
            prices_in[role] = prices_out[role]
            for copy in price_copies:
                copy.wait()
            for d in range(districts):
                gradient = costs_ref[d].astype(F32) + mm(chosen_in[d], coupling[d])
                plan_ref[d] = -mm(gradient.astype(BF16), factor[d])
            for copy in dual_copies:
                copy.wait()
            prices_ref[...] = prices_in[...]
        moved = take_draws(outer, copies)
    duals_ref[...] = (duals[...] + moved)[:, :horizon]
    for send in sends:
        send.wait_send()


def handover(plan_ref, prices_ref, duals_ref, plan_out, prices_out, duals_out, sem):
    copies = [
        pltpu.make_async_copy(source, target, sem.at[index])
        for index, (source, target) in enumerate(
            ((plan_ref, plan_out), (prices_ref, prices_out), (duals_ref, duals_out))
        )
    ]
    for copy in copies:
        copy.start()
    for copy in copies:
        copy.wait()


def on_device(cost_terms, neighbours, relayout, ownership, capacity, coupling, solve_factor):
    districts, rows, unknowns = cost_terms.shape
    interface = coupling.shape[2]
    group = relayout.shape[1]
    sub_count = lax.axis_size("sub")
    district_count = lax.axis_size("district")
    load_count = districts * district_count * group // (2 * RESERVOIRS)
    dual_scale = reserve_step / math.sqrt(load_count)
    near = neighbours.transpose(0, 2, 1).reshape(districts * LINK_COUNT, rows)
    coupling = coupling.transpose(0, 2, 1)
    block = districts * rows
    blocks = group // block
    window = block + 2 * HALO
    vmem = pl.BlockSpec(memory_space=pltpu.VMEM)
    hbm = pl.BlockSpec(memory_space=pl.ANY)
    dma = pltpu.SemaphoreType.DMA
    results = pl.pallas_call(
        functools.partial(kernel, dual_scale),
        name="districts",
        out_shape=(
            jax.ShapeDtypeStruct((districts, rows, unknowns), F32),
            jax.ShapeDtypeStruct((districts, rows, interface), F32),
            jax.ShapeDtypeStruct(capacity.shape, F32),
        ),
        in_specs=[pl.BlockSpec(memory_space=pltpu.HBM)] * 7,
        out_specs=(vmem, vmem, vmem),
        scratch_shapes=[
            pltpu.VMEM(cost_terms.shape, BF16),
            pltpu.VMEM(near.shape, jnp.int32),
            pltpu.VMEM(ownership.shape, jnp.int32),
            pltpu.VMEM(relayout.shape, jnp.int32),
            pltpu.VMEM(capacity.shape, F32),
            pltpu.VMEM(coupling.shape, BF16),
            pltpu.VMEM(solve_factor.shape, BF16),
            pltpu.VMEM((districts, LINK_COUNT, LANES), jnp.int32),
            pltpu.VMEM((sub_count, LINK_COUNT, LANES), jnp.int32),
            pltpu.VMEM((LINK_COUNT, group + 2 * HALO), jnp.int32),
            pltpu.VMEM((1, group), jnp.int32),
            pltpu.VMEM((rows, 2 * LANES), F32),
            pltpu.VMEM((districts, rows + rows // 2, LANES), BF16),
            pltpu.VMEM((sub_count, rows + rows // 2, LANES), BF16),
            pltpu.VMEM((group, 2 * LANES), BF16),
            pltpu.VMEM((group, interface), F32),
            pltpu.VMEM((group, interface), F32),
            pltpu.VMEM((group + 2 * HALO, interface), BF16),
            pltpu.VMEM((window, interface), F32),
            pltpu.VMEM((blocks, block, window), BF16),
            pltpu.VMEM((interface, interface), BF16),
            pltpu.VMEM((group, RESERVOIRS), BF16),
            pltpu.VMEM((RESERVOIRS, group), BF16),
            pltpu.VMEM((blocks, block, block), BF16),
            pltpu.VMEM((block, window), BF16),
            pltpu.VMEM((districts, rows, interface), BF16),
            pltpu.VMEM((districts, rows, interface), BF16),
            pltpu.VMEM((districts, rows, interface), F32),
            pltpu.VMEM((districts, rows, interface), F32),
            pltpu.VMEM((RESERVOIRS, LANES), F32),
            pltpu.VMEM((OUTER_ITERS, RESERVOIRS, LANES), F32),
            pltpu.VMEM((OUTER_ITERS, district_count * districts, RESERVOIRS, LANES), F32),
            dma((2 * districts + 5,)),
            dma((sub_count,)),
            dma((sub_count,)),
            dma((sub_count,)),
            dma((sub_count,)),
            dma((OUTER_ITERS, district_count * districts)),
            dma((OUTER_ITERS, district_count * districts)),
            dma((districts,)),
            dma((districts,)),
            dma((districts,)),
            dma((districts,)),
        ],
        compiler_params=pltpu.CompilerParams(
            collective_id=0, has_side_effects=True, vmem_limit_bytes=(20 if group <= 1024 else 60) * 1024 * 1024
        ),
    )(*[pltpu.with_memory_space_constraint(value, pltpu.HBM) for value in (cost_terms, near, ownership, relayout, capacity, coupling, solve_factor)])
    return pl.pallas_call(
        handover,
        name="handover",
        out_shape=tuple(jax.ShapeDtypeStruct(value.shape, value.dtype) for value in results),
        in_specs=[hbm] * 3,
        out_specs=(hbm,) * 3,
        scratch_shapes=[dma((3,))],
        compiler_params=pltpu.CompilerParams(vmem_limit_bytes=4 * 1024 * 1024),
    )(*results)


def solution(mesh):
    placed = (
        P("district", "sub", None),
        P("district", "sub", None),
        P("district", None),
        P("district", "sub"),
        P(),
        P("district", None, None),
        P("district", None, None),
    )
    return jax.shard_map(
        on_device,
        mesh=mesh,
        in_specs=placed,
        out_specs=(P("district", "sub", None), P("district", "sub", None), P()),
        check_vma=False,
    )
```

```python
import functools
import math

import jax
import jax.numpy as jnp
from jax import lax
from jax.experimental import pallas as pl
from jax.experimental.pallas import tpu as pltpu
from jax.sharding import PartitionSpec as P

REACH_SPAN = 16
LINK_COUNT = 4
RESERVOIRS = 16
OUTER_ITERS = 2
INNER_ITERS = 4
HALO = 2 * REACH_SPAN
LANES = 128

price_step = 0.3
reserve_step = 1.0

F32 = jnp.float32
BF16 = jnp.bfloat16
MESH = pl.DeviceIdType.MESH


def each(count, body):
    if count <= 8:
        for index in range(count):
            body(index)
    else:
        lax.fori_loop(0, count, lambda index, carry: (body(index), carry)[1], 0)


def mm(a, b):
    return jnp.dot(a, b, preferred_element_type=F32)


def contract(a, b, dim):
    return lax.dot_general(a, b, (((dim,), (dim,)), ((), ())), preferred_element_type=F32)


def fold(wide, half):
    tail = wide[:, LANES:]
    lane = lax.broadcasted_iota(jnp.int32, (half, LANES), 1)
    folded = jnp.where(lane < LANES // 2, tail[:half], pltpu.roll(tail[half:], LANES // 2, 1))
    return jnp.concatenate([wide[:, :LANES], folded], axis=0)


def unfold(folded, rows):
    tail = folded[rows:]
    return jnp.concatenate([tail, pltpu.roll(tail, LANES // 2, 1)], axis=0)


def unfolded(folded, rows):
    return jnp.concatenate([folded[:rows], unfold(folded, rows)], axis=1)


def response(powers):
    shift, summed = [], []
    for i in range(INNER_ITERS):
        chosen, added = 0.0, 0.0
        for j in range(i, INNER_ITERS):
            scale = price_step ** j
            chosen = chosen + scale * math.comb(INNER_ITERS - 1, i) * math.comb(INNER_ITERS - 1 - i, j - i) * powers[j]
            weight = sum(math.comb(k, i) * math.comb(k - i, j - i) for k in range(j, INNER_ITERS))
            added = added + price_step * scale * weight * powers[j + 1]
        shift.append(chosen)
        summed.append(added)
    return jnp.concatenate(shift, axis=0), jnp.concatenate(summed, axis=0)


def target_of(index, me, count):
    low = 1 - jnp.minimum(me // (count // 2), 1)
    climb = index + jnp.minimum(jnp.maximum(index - me + 1, 0), 1)
    fall = count - 1 - index
    fall = fall - jnp.minimum(jnp.maximum(me - fall + 1, 0), 1)
    return low * fall + (1 - low) * climb


def kernel(
    dual_scale, costs_hbm, near_hbm, owner_hbm, relayout_hbm, capacity_hbm, coupling_hbm, factor_hbm,
    plan_ref, prices_ref, duals_ref,
    costs_ref, near_ref, owner_ref, relayout_ref, capacity_ref, coupling, factor, tables, near, links, owners, wide_first, first, landed, gathered, base, state, flow, total, spread, inner, weight, answer, answer_sum, reply, replies,
    match_t, select, near_links, factors_out, factors_in, chosen_out, chosen_in, prices_out, prices_in, duals, draws, arrived,
    local_sem, near_send, near_recv, flow_send, flow_recv, draw_send, draw_recv, reply_send, reply_recv,
    factors_send, factors_recv, price_send, price_recv, dual_send, dual_recv,
):
    districts, rows, unknowns = costs_ref.shape
    interface = coupling.shape[1]
    horizon = capacity_ref.shape[1]
    group = relayout_ref.shape[1]
    sub_count = lax.axis_size("sub")
    district_count = lax.axis_size("district")
    me = lax.axis_index("sub")
    role = lax.rem(me, districts)
    team = me // districts * districts
    my_district = lax.axis_index("district")
    block = districts * rows
    window = block + 2 * HALO
    blocks = group // block

    costs_load = pltpu.make_async_copy(costs_hbm, costs_ref, local_sem.at[2 * districts])
    costs_load.start()
    loads = []
    for d in range(districts):
        loads.append(
            (
                pltpu.make_async_copy(factor_hbm.at[d], factor.at[d], local_sem.at[2 * d]),
                pltpu.make_async_copy(coupling_hbm.at[d], coupling.at[d], local_sem.at[2 * d + 1]),
            )
        )
        for load in loads[-1]:
            load.start()

    small_loads = [
        pltpu.make_async_copy(source, target, local_sem.at[2 * districts + 1 + index])
        for index, (source, target) in enumerate(
            (
                (near_hbm, near_ref),
                (owner_hbm, owner_ref),
                (relayout_hbm, relayout_ref),
                (capacity_hbm, capacity_ref),
            )
        )
    ]
    for load in small_loads:
        load.start()

    barrier = pltpu.get_barrier_semaphore()
    for step in range(1, sub_count):
        pl.semaphore_signal(
            barrier, inc=1, device_id={"sub": lax.rem(me + step, sub_count)}, device_id_type=MESH
        )
    for step in range(1, district_count):
        for other in range(districts):
            pl.semaphore_signal(
                barrier,
                inc=1,
                device_id={
                    "district": lax.rem(my_district + step, district_count),
                    "sub": team + lax.rem(role + other, districts),
                },
                device_id_type=MESH,
            )

    costs_load.wait()
    for d in range(districts):
        for load in loads[d]:
            load.wait()
        first_plan = -mm(costs_ref[d], factor[d])
        plan_ref[d] = first_plan
        wide_first[:, :interface] = contract(first_plan.astype(BF16), coupling[d], 1)
        first[d] = fold(wide_first[...], rows // 2).astype(BF16)

    for load in small_loads:
        load.wait()
    for d in range(districts):
        for k in range(LINK_COUNT):
            tables[d, k // 2 : k // 2 + 1, k % 2 * rows : (k % 2 + 1) * rows] = near_ref[d * LINK_COUNT + k : d * LINK_COUNT + k + 1, :]
        tables[d, LINK_COUNT // 2 : LINK_COUNT // 2 + 1, :rows] = owner_ref[d : d + 1, :]
    pl.semaphore_wait(barrier, sub_count - 1 + (district_count - 1) * districts)
    sends = []
    for index in range(sub_count - 1):
        target = target_of(index, me, sub_count)
        sends.append(
            pltpu.make_async_remote_copy(
                src_ref=tables.at[lax.rem(target, districts)],
                dst_ref=near.at[me],
                send_sem=near_send.at[index],
                recv_sem=near_recv.at[me],
                device_id={"sub": target},
                device_id_type=MESH,
            )
        )
        sends[-1].start()
    for index in range(sub_count - 1):
        target = target_of(index, me, sub_count)
        sends.append(
            pltpu.make_async_remote_copy(
                src_ref=first.at[lax.rem(target, districts)],
                dst_ref=landed.at[me],
                send_sem=flow_send.at[index],
                recv_sem=flow_recv.at[me],
                device_id={"sub": target},
                device_id_type=MESH,
            )
        )
        sends[-1].start()

    landed[me] = first[role]
    for d in range(districts):
        inner[d] = mm(coupling[d], factor[d]).astype(BF16)
        weight[d] = jnp.zeros_like(weight[d])
        weight[d, :, :interface] = (-contract(inner[d], coupling[d], 1)).astype(BF16)

    pitch = 2 * LANES // INNER_ITERS
    row = lax.broadcasted_iota(jnp.int32, (pitch, 2 * LANES), 0)
    column = lax.broadcasted_iota(jnp.int32, (pitch, 2 * LANES), 1)
    powers = [[jnp.where((row == column) & (row < horizon), 1.0, 0.0)] for _ in range(districts)]
    for d in range(districts):
        powers[d].append(jnp.where(row < horizon, weight[d, :pitch, :].astype(F32), 0.0))
    for _ in range(INNER_ITERS - 1):
        for d in range(districts):
            last = powers[d][-1][:, :interface]
            high = last.astype(BF16)
            low = (last - high.astype(F32)).astype(BF16)
            both = mm(jnp.concatenate([high, low], axis=0), weight[d])
            powers[d].append(both[:pitch] + both[pitch:])
    replied = []
    for d in range(districts):
        chosen, added = response(powers[d])
        answer[d] = chosen.astype(BF16)
        answer_sum[d] = added.astype(BF16)
        reply[d] = response(powers[d][1:] + powers[d][:1])[0][:, :LANES].T[:horizon].astype(BF16)

    partners = [
        (step, other)
        for step in range(district_count)
        for other in range(districts)
        if step or other
    ]

    def partner(step, other):
        return {
            "district": lax.rem(my_district + step, district_count),
            "sub": team + lax.rem(role + other, districts),
        }

    reply_copies = []
    for index, (step, other) in enumerate(partners):
        reply_copies.append(
            pltpu.make_async_remote_copy(
                src_ref=reply.at[role],
                dst_ref=replies.at[index],
                send_sem=reply_send.at[index],
                recv_sem=reply_recv.at[index],
                device_id=partner(step, other),
                device_id_type=MESH,
            )
        )
        reply_copies[-1].start()

    moves = relayout_ref[pl.ds(role, 1), :]
    team_rows = districts * rows
    pick = lax.broadcasted_iota(jnp.int32, (team_rows, group), 1) == (
        lax.broadcasted_iota(jnp.int32, (team_rows, group), 0) + team * rows
    )
    pick = jnp.where(pick, 1.0, 0.0).astype(BF16)

    def choose(b):
        place = lax.broadcasted_iota(jnp.int32, (block, group), 0) + b * block
        chosen = jnp.where(place == moves, 1.0, 0.0).astype(BF16)
        select[b] = contract(pick, chosen, 1).astype(BF16)

    each(blocks, choose)

    duals[...] = jnp.zeros_like(duals)
    duals[:, :horizon] = capacity_ref[...]
    capacity = duals[...]
    flow[...] = jnp.zeros_like(flow)
    links[...] = jnp.full_like(links, -window * 4)

    near[me] = tables[role]
    for step in range(1, sub_count):
        source = lax.rem(me + step, sub_count)
        pltpu.make_async_remote_copy(
            src_ref=tables.at[role],
            dst_ref=near.at[source],
            send_sem=near_send.at[step - 1],
            recv_sem=near_recv.at[source],
            device_id={"sub": source},
            device_id_type=MESH,
        ).wait_recv()
    for source in range(sub_count):
        for k in range(LINK_COUNT):
            links[k : k + 1, HALO + source * rows : HALO + (source + 1) * rows] = near[source, k // 2 : k // 2 + 1, k % 2 * rows : (k % 2 + 1) * rows]
        owners[:, source * rows : (source + 1) * rows] = near[source, LINK_COUNT // 2 : LINK_COUNT // 2 + 1, :rows]
    own = owners[...]
    held = lax.broadcasted_iota(jnp.int32, (RESERVOIRS, group), 0)
    match_t[...] = jnp.where(held == own, 1.0, 0.0).astype(BF16)
    edge = interface - LANES
    held = lax.broadcasted_iota(jnp.int32, (LANES, group), 0) - edge
    base[:, LANES:] = jnp.where((held == own) & (held >= 0) & (held < RESERVOIRS), 1.0, 0.0).T

    def linked(start, width):
        column = lax.broadcasted_iota(jnp.int32, (width, width), 0)
        row = lax.broadcasted_iota(jnp.int32, (width, width), 1)
        table = jnp.where(column == row, 1.0, 0.0)
        for k in range(LINK_COUNT):
            link = links[k : k + 1, pl.ds(start, width)] - (start - HALO)
            table = table - jnp.where(column == link, 1.0 / LINK_COUNT, 0.0)
        return table.T.astype(BF16)

    def build(b):
        start = b * block if isinstance(b, int) else pl.multiple_of(b * block, block)
        table = linked(start, window)
        spread[b] = mm(table[HALO : HALO + block], table).astype(BF16)

    each(blocks, build)
    near_links[...] = linked(pl.multiple_of(team * rows, team_rows), window)[HALO : HALO + team_rows]

    for step in range(1, sub_count):
        source = lax.rem(me + step, sub_count)
        pltpu.make_async_remote_copy(
            src_ref=first.at[role],
            dst_ref=landed.at[source],
            send_sem=flow_send.at[step - 1],
            recv_sem=flow_recv.at[source],
            device_id={"sub": source},
            device_id_type=MESH,
        ).wait_recv()

    def spread_out(source):
        at = pl.ds(source * rows, rows)
        gathered[at, :LANES] = landed[source, :rows, :]
        gathered[at, LANES:] = unfold(landed[source].astype(F32), rows).astype(BF16)

    each(sub_count, spread_out)

    def at_block(b, extra=0, size=block):
        return pl.ds(b * block + extra, size)

    lane = lax.broadcasted_iota(jnp.int32, (block, LANES), 1)

    def permute(b):
        place = lax.broadcasted_iota(jnp.int32, (block, group), 0) + b * block
        chosen = jnp.where(place == moves, 1.0, 0.0).astype(BF16)
        moved = mm(chosen, gathered[...])
        tail = jnp.where(lane < edge, moved[:, LANES:], base[at_block(b), LANES:])
        base[at_block(b), :LANES] = moved[:, :LANES]
        base[at_block(b), LANES:] = tail
        flow[at_block(b, HALO), :LANES] = moved[:, :LANES].astype(BF16)
        flow[at_block(b, HALO), LANES:] = tail.astype(BF16)

    each(blocks, permute)

    team_window = pl.ds(pl.multiple_of(team * rows, team_rows), window)
    total[...] = flow[team_window, :].astype(F32)

    def forward():
        def one(b):
            price = state[at_block(b), :].astype(BF16)
            flow[at_block(b, HALO), :] = (base[at_block(b), :] + mm(price, weight[role])).astype(BF16)

        each(blocks, one)
        total[...] += flow[team_window, :].astype(F32)

    def backward(fresh=False, grow=False):
        def one(b):
            out = mm(spread[b], flow[at_block(b, 0, window), :])
            gain = price_step * out[:, :interface]
            state[at_block(b), :] = gain if fresh else state[at_block(b), :] + gain
            if grow:
                tail = base[at_block(b), LANES:]
                base[at_block(b), LANES:] = jnp.where(
                    lane < edge + RESERVOIRS, tail, pltpu.roll(out[:, LANES:] - tail, RESERVOIRS, 1)
                )

        each(blocks, one)

    def send_draws(outer):
        drawn = mm(match_t[...], flow[HALO : HALO + group, :])
        side = lax.broadcasted_iota(jnp.int32, (RESERVOIRS, LANES), 1)
        draws[outer] = jnp.where(side < edge, drawn[:, :LANES], drawn[:, LANES:])
        copies = []
        for index, (step, other) in enumerate(partners):
            copies.append(
                pltpu.make_async_remote_copy(
                    src_ref=draws.at[outer],
                    dst_ref=arrived.at[outer, index],
                    send_sem=draw_send.at[outer, index],
                    recv_sem=draw_recv.at[outer, index],
                    device_id=partner(step, other),
                    device_id_type=MESH,
                )
            )
            copies[-1].start()
        return copies

    def take_draws(outer, copies):
        drawn = draws[outer]
        for index, copy in enumerate(copies):
            copy.wait()
            drawn = drawn + arrived[outer, index]
        return drawn

    def to_team(source_ref, place_ref, send_sem, recv_sem):
        copies = []
        for other in range(1, districts):
            target = lax.rem(role + other, districts)
            copies.append(
                pltpu.make_async_remote_copy(
                    src_ref=source_ref.at[target],
                    dst_ref=place_ref.at[role],
                    send_sem=send_sem.at[other],
                    recv_sem=recv_sem.at[other],
                    device_id={"sub": team + target},
                    device_id_type=MESH,
                )
            )
            copies[-1].start()
        place_ref[role] = source_ref[role]
        return copies

    def chosen_rows(values):
        chosen = mm(select[0], values(0))
        for b in range(1, blocks):
            chosen = chosen + mm(select[b], values(b))
        return chosen

    backward(fresh=True, grow=True)
    for step in range(1, INNER_ITERS - 1):
        forward()
        backward(grow=True)
    forward()
    copies = send_draws(0)

    picked = chosen_rows(lambda b: flow[at_block(b, HALO), LANES:])
    local = mm(near_links[...], flow[team_window, LANES:])
    factors = jnp.where(lane < LANES // 2, pltpu.roll(picked, LANES // 2, 1), local)
    factors_out[...] = factors.reshape(districts, rows, LANES).astype(BF16)
    factor_copies = to_team(factors_out, factors_in, factors_send, factors_recv)

    backward()
    for step in range(INNER_ITERS - 1):
        forward()
        backward()
    chosen = chosen_rows(lambda b: state[at_block(b), :].astype(BF16))
    for d in range(districts):
        wide_first[:, :interface] = chosen[d * rows : (d + 1) * rows]
        chosen_out[d] = fold(wide_first[...], rows // 2).astype(BF16)
    price_copies = to_team(chosen_out, chosen_in, price_send, price_recv)
    forward()
    late_copies = send_draws(1)
    high = total[...].astype(BF16)
    low = (total[...] - high.astype(F32)).astype(BF16)
    prices = price_step * (mm(near_links[...], high) + mm(near_links[...], low))
    for d in range(districts):
        prices_out[d] = fold(prices[d * rows : (d + 1) * rows], rows // 2).astype(BF16)
    dual_copies = to_team(prices_out, prices_in, dual_send, dual_recv)

    drawn = take_draws(0, copies)
    side = lax.broadcasted_iota(jnp.int32, drawn.shape, 1)
    moved = jnp.where(side < horizon, (drawn - capacity) * dual_scale, 0.0)
    half = pltpu.roll(moved, pitch, 1)
    none = jnp.zeros_like(moved)
    steps = jnp.concatenate(
        [
            jnp.concatenate([moved, none], axis=1),
            jnp.concatenate([half, none], axis=1),
            jnp.concatenate([none, moved], axis=1),
            jnp.concatenate([none, half], axis=1),
        ],
        axis=0,
    ).astype(BF16)
    for copy in factor_copies:
        copy.wait()
    blank = jnp.zeros_like(steps)
    pair = jnp.concatenate(
        [jnp.concatenate([steps, blank], axis=1), jnp.concatenate([blank, steps], axis=1)], axis=0
    )
    price_change, dual_change = [], []
    for d in range(districts):
        change = mm(factors_in[d], pair).astype(BF16)
        price_change.append(mm(change[:, : 2 * LANES], answer[d]))
        dual_change.append(mm(change[:, 2 * LANES :], answer_sum[d]))

    heard = [draws[0]] + [arrived[0, index] for index in range(len(partners))]
    for copy in reply_copies:
        copy.wait()
    returns = mm(jnp.concatenate(heard, axis=0)[:, LANES // 2 :].astype(BF16), steps).astype(BF16)
    late = contract(returns[:RESERVOIRS], reply[role], 1)
    for index in range(len(partners)):
        at = slice((index + 1) * RESERVOIRS, (index + 2) * RESERVOIRS)
        late = late + contract(returns[at], replies[index], 1)

    for copy in price_copies:
        copy.wait()
    for d in range(districts):
        price = unfolded(chosen_in[d].astype(F32), rows)[:, :interface] + price_change[d][:, :interface]
        plan_ref[d] = plan_ref[d] - mm(price.astype(BF16), inner[d])
    for copy in dual_copies:
        copy.wait()
    for d in range(districts):
        prices_ref[d] = unfolded(prices_in[d].astype(F32), rows)[:, :interface] + dual_change[d][:, :interface]
    drawn = take_draws(1, late_copies)
    duals_ref[...] = moved[:, :horizon] + ((drawn[:, :horizon] + late) - capacity[:, :horizon]) * dual_scale
    for send in sends:
        send.wait_send()


def handover(plan_ref, prices_ref, duals_ref, plan_out, prices_out, duals_out, sem):
    copies = [
        pltpu.make_async_copy(source, target, sem.at[index])
        for index, (source, target) in enumerate(
            ((plan_ref, plan_out), (prices_ref, prices_out), (duals_ref, duals_out))
        )
    ]
    for copy in copies:
        copy.start()
    for copy in copies:
        copy.wait()


def on_device(cost_terms, neighbours, relayout, ownership, capacity, coupling, solve_factor):
    districts, rows, unknowns = cost_terms.shape
    interface = coupling.shape[2]
    group = relayout.shape[1]
    sub_count = lax.axis_size("sub")
    district_count = lax.axis_size("district")
    load_count = districts * district_count * group // (2 * RESERVOIRS)
    dual_scale = reserve_step / math.sqrt(load_count)
    near = neighbours.transpose(0, 2, 1).reshape(districts * LINK_COUNT, rows)
    coupling = coupling.transpose(0, 2, 1)
    block = districts * rows
    blocks = group // block
    window = block + 2 * HALO
    vmem = pl.BlockSpec(memory_space=pltpu.VMEM)
    hbm = pl.BlockSpec(memory_space=pl.ANY)
    dma = pltpu.SemaphoreType.DMA
    results = pl.pallas_call(
        functools.partial(kernel, dual_scale),
        name="districts",
        out_shape=(
            jax.ShapeDtypeStruct((districts, rows, unknowns), F32),
            jax.ShapeDtypeStruct((districts, rows, interface), F32),
            jax.ShapeDtypeStruct(capacity.shape, F32),
        ),
        in_specs=[pl.BlockSpec(memory_space=pltpu.HBM)] * 7,
        out_specs=(vmem, vmem, vmem),
        scratch_shapes=[
            pltpu.VMEM(cost_terms.shape, BF16),
            pltpu.VMEM(near.shape, jnp.int32),
            pltpu.VMEM(ownership.shape, jnp.int32),
            pltpu.VMEM(relayout.shape, jnp.int32),
            pltpu.VMEM(capacity.shape, F32),
            pltpu.VMEM(coupling.shape, BF16),
            pltpu.VMEM(solve_factor.shape, BF16),
            pltpu.VMEM((districts, LINK_COUNT, LANES), jnp.int32),
            pltpu.VMEM((sub_count, LINK_COUNT, LANES), jnp.int32),
            pltpu.VMEM((LINK_COUNT, group + 2 * HALO), jnp.int32),
            pltpu.VMEM((1, group), jnp.int32),
            pltpu.VMEM((rows, 2 * LANES), F32),
            pltpu.VMEM((districts, rows + rows // 2, LANES), BF16),
            pltpu.VMEM((sub_count, rows + rows // 2, LANES), BF16),
            pltpu.VMEM((group, 2 * LANES), BF16),
            pltpu.VMEM((group, 2 * LANES), F32),
            pltpu.VMEM((group, interface), F32),
            pltpu.VMEM((group + 2 * HALO, 2 * LANES), BF16),
            pltpu.VMEM((window, 2 * LANES), F32),
            pltpu.VMEM((blocks, block, window), BF16),
            pltpu.VMEM((districts, interface, unknowns), BF16),
            pltpu.VMEM((districts, interface, 2 * LANES), BF16),
            pltpu.VMEM((districts, 2 * LANES, 2 * LANES), BF16),
            pltpu.VMEM((districts, 2 * LANES, 2 * LANES), BF16),
            pltpu.VMEM((districts, capacity.shape[1], 2 * LANES), BF16),
            pltpu.VMEM((district_count * districts, capacity.shape[1], 2 * LANES), BF16),
            pltpu.VMEM((RESERVOIRS, group), BF16),
            pltpu.VMEM((blocks, block, block), BF16),
            pltpu.VMEM((block, window), BF16),
            pltpu.VMEM((districts, rows, LANES), BF16),
            pltpu.VMEM((districts, rows, LANES), BF16),
            pltpu.VMEM((districts, rows + rows // 2, LANES), BF16),
            pltpu.VMEM((districts, rows + rows // 2, LANES), BF16),
            pltpu.VMEM((districts, rows + rows // 2, LANES), BF16),
            pltpu.VMEM((districts, rows + rows // 2, LANES), BF16),
            pltpu.VMEM((RESERVOIRS, LANES), F32),
            pltpu.VMEM((OUTER_ITERS, RESERVOIRS, LANES), F32),
            pltpu.VMEM((OUTER_ITERS, district_count * districts, RESERVOIRS, LANES), F32),
            dma((2 * districts + 5,)),
            dma((sub_count,)),
            dma((sub_count,)),
            dma((sub_count,)),
            dma((sub_count,)),
            dma((OUTER_ITERS, district_count * districts)),
            dma((OUTER_ITERS, district_count * districts)),
            dma((district_count * districts,)),
            dma((district_count * districts,)),
            dma((districts,)),
            dma((districts,)),
            dma((districts,)),
            dma((districts,)),
            dma((districts,)),
            dma((districts,)),
        ],
        compiler_params=pltpu.CompilerParams(
            collective_id=0, has_side_effects=True, vmem_limit_bytes=(20 if group <= 1024 else 60) * 1024 * 1024
        ),
    )(*[pltpu.with_memory_space_constraint(value, pltpu.HBM) for value in (cost_terms, near, ownership, relayout, capacity, coupling, solve_factor)])
    return pl.pallas_call(
        handover,
        name="handover",
        out_shape=tuple(jax.ShapeDtypeStruct(value.shape, value.dtype) for value in results),
        in_specs=[hbm] * 3,
        out_specs=(hbm,) * 3,
        scratch_shapes=[dma((3,))],
        compiler_params=pltpu.CompilerParams(vmem_limit_bytes=4 * 1024 * 1024),
    )(*results)


def solution(mesh):
    placed = (
        P("district", "sub", None),
        P("district", "sub", None),
        P("district", None),
        P("district", "sub"),
        P(),
        P("district", None, None),
        P("district", None, None),
    )
    return jax.shard_map(
        on_device,
        mesh=mesh,
        in_specs=placed,
        out_specs=(P("district", "sub", None), P("district", "sub", None), P()),
        check_vma=False,
    )
```

```python
import functools
import math

import jax
import jax.numpy as jnp
from jax import lax
from jax.experimental import pallas as pl
from jax.experimental.pallas import tpu as pltpu
from jax.sharding import PartitionSpec as P

REACH_SPAN = 16
LINK_COUNT = 4
RESERVOIRS = 16
OUTER_ITERS = 2
INNER_ITERS = 4
HALO = 2 * REACH_SPAN
LANES = 128

price_step = 0.3
reserve_step = 1.0

F32 = jnp.float32
BF16 = jnp.bfloat16
MESH = pl.DeviceIdType.MESH


def each(count, body):
    if count <= 8:
        for index in range(count):
            body(index)
    else:
        lax.fori_loop(0, count, lambda index, carry: (body(index), carry)[1], 0)


def mm(a, b):
    return jnp.dot(a, b, preferred_element_type=F32)


def contract(a, b, dim):
    return lax.dot_general(a, b, (((dim,), (dim,)), ((), ())), preferred_element_type=F32)


def fold(wide, half):
    tail = wide[:, LANES:]
    lane = lax.broadcasted_iota(jnp.int32, (half, LANES), 1)
    folded = jnp.where(lane < LANES // 2, tail[:half], pltpu.roll(tail[half:], LANES // 2, 1))
    return jnp.concatenate([wide[:, :LANES], folded], axis=0)


def unfold(folded, rows):
    tail = folded[rows:]
    return jnp.concatenate([tail, pltpu.roll(tail, LANES // 2, 1)], axis=0)


def unfolded(folded, rows):
    return jnp.concatenate([folded[:rows], unfold(folded, rows)], axis=1)


def response(powers):
    shift, summed = [], []
    for i in range(INNER_ITERS):
        chosen, added = 0.0, 0.0
        for j in range(i, INNER_ITERS):
            scale = price_step ** j
            chosen = chosen + scale * math.comb(INNER_ITERS - 1, i) * math.comb(INNER_ITERS - 1 - i, j - i) * powers[j]
            weight = sum(math.comb(k, i) * math.comb(k - i, j - i) for k in range(j, INNER_ITERS))
            added = added + price_step * scale * weight * powers[j + 1]
        shift.append(chosen)
        summed.append(added)
    return jnp.concatenate(shift, axis=0), jnp.concatenate(summed, axis=0)


def whole_wait(place_ref, start, count, send_sem, recv_sem, device):
    places = place_ref.at[pl.ds(start, count)]
    return pltpu.make_async_remote_copy(
        src_ref=places, dst_ref=places, send_sem=send_sem, recv_sem=recv_sem, device_id=device, device_id_type=MESH
    )


def target_of(index, me, count, width):
    place, turn = me // width, lax.rem(me, width)
    pairs = count // width
    if index >= count - width:
        return place * width + lax.rem(turn + 1 + index - (count - width), width)
    slot = index // width
    low = 1 - jnp.minimum(place // (pairs // 2), 1)
    climb = slot + jnp.minimum(jnp.maximum(slot - place + 1, 0), 1)
    fall = pairs - 1 - slot
    fall = fall - jnp.minimum(jnp.maximum(place - fall + 1, 0), 1)
    return (low * fall + (1 - low) * climb) * width + lax.rem(turn + 1 + index % width, width)


def kernel(
    dual_scale, costs_hbm, near_hbm, owner_hbm, relayout_hbm, capacity_hbm, coupling_hbm, factor_hbm,
    plan_ref, prices_ref, duals_ref,
    costs_ref, near_ref, owner_ref, relayout_ref, capacity_ref, coupling, factor, tables, near, links, owners, wide_first, first, landed, gathered, base, state, flow, total, spread, inner, weight, answer, answer_sum, reply, replies,
    match_t, owned, onehot, select, near_links, factors_out, factors_in, chosen_out, chosen_in, prices_out, prices_in, duals, draws, arrived, returned, returning,
    local_sem, near_send, near_recv, flow_send, flow_recv, draw_send, draw_recv, reply_send, reply_recv, return_send, return_recv,
    factors_send, factors_recv, price_send, price_recv, dual_send, dual_recv,
):
    districts, rows, unknowns = costs_ref.shape
    interface = coupling.shape[1]
    horizon = capacity_ref.shape[1]
    group = relayout_ref.shape[1]
    sub_count = lax.axis_size("sub")
    district_count = lax.axis_size("district")
    me = lax.axis_index("sub")
    role = lax.rem(me, districts)
    team = me // districts * districts
    my_district = lax.axis_index("district")
    block = districts * rows
    window = block + 2 * HALO
    blocks = group // block

    costs_load = pltpu.make_async_copy(costs_hbm, costs_ref, local_sem.at[2 * districts])
    costs_load.start()
    loads = []
    for d in range(districts):
        loads.append(
            (
                pltpu.make_async_copy(factor_hbm.at[d], factor.at[d], local_sem.at[2 * d]),
                pltpu.make_async_copy(coupling_hbm.at[d], coupling.at[d], local_sem.at[2 * d + 1]),
            )
        )
        for load in loads[-1]:
            load.start()

    small_loads = [
        pltpu.make_async_copy(source, target, local_sem.at[2 * districts + 1 + index])
        for index, (source, target) in enumerate(
            (
                (near_hbm, near_ref),
                (owner_hbm, owner_ref),
                (relayout_hbm, relayout_ref),
                (capacity_hbm, capacity_ref),
            )
        )
    ]
    for load in small_loads:
        load.start()

    barrier = pltpu.get_barrier_semaphore()
    for step in range(1, sub_count):
        pl.semaphore_signal(
            barrier, inc=1, device_id={"sub": lax.rem(me + step, sub_count)}, device_id_type=MESH
        )
    for step in range(1, district_count):
        for other in range(districts):
            pl.semaphore_signal(
                barrier,
                inc=1,
                device_id={
                    "district": lax.rem(my_district + step, district_count),
                    "sub": team + lax.rem(role + other, districts),
                },
                device_id_type=MESH,
            )

    costs_load.wait()
    for d in range(districts):
        for load in loads[d]:
            load.wait()
        first_plan = -mm(costs_ref[d], factor[d])
        plan_ref[d] = first_plan
        wide_first[:, :interface] = contract(first_plan.astype(BF16), coupling[d], 1)
        first[d] = fold(wide_first[...], rows // 2).astype(BF16)

    for load in small_loads:
        load.wait()
    for d in range(districts):
        for k in range(LINK_COUNT):
            tables[d, k // 2 : k // 2 + 1, k % 2 * rows : (k % 2 + 1) * rows] = near_ref[d * LINK_COUNT + k : d * LINK_COUNT + k + 1, :]
        tables[d, LINK_COUNT // 2 : LINK_COUNT // 2 + 1, :rows] = owner_ref[d : d + 1, :]
    pl.semaphore_wait(barrier, sub_count - 1 + (district_count - 1) * districts)
    beside = {"sub": lax.rem(me + 1, sub_count)}
    near_all = whole_wait(near, 0, sub_count - 1, near_send.at[0], near_recv.at[0], beside)
    flow_all = whole_wait(landed, 0, sub_count - 1, flow_send.at[0], flow_recv.at[0], beside)
    sends = []
    for index in range(sub_count - 1):
        target = target_of(index, me, sub_count, districts)
        sends.append(
            pltpu.make_async_remote_copy(
                src_ref=tables.at[lax.rem(target, districts)],
                dst_ref=near.at[me],
                send_sem=near_send.at[0],
                recv_sem=near_recv.at[0],
                device_id={"sub": target},
                device_id_type=MESH,
            )
        )
        sends[-1].start()
    for index in range(sub_count - 1):
        target = target_of(index, me, sub_count, districts)
        sends.append(
            pltpu.make_async_remote_copy(
                src_ref=first.at[lax.rem(target, districts)],
                dst_ref=landed.at[me],
                send_sem=flow_send.at[0],
                recv_sem=flow_recv.at[0],
                device_id={"sub": target},
                device_id_type=MESH,
            )
        )
        sends[-1].start()

    landed[me] = first[role]
    for d in range(districts):
        inner[d] = mm(coupling[d], factor[d]).astype(BF16)
        weight[d] = jnp.zeros_like(weight[d])
        weight[d, :, :interface] = (-contract(inner[d], coupling[d], 1)).astype(BF16)

    pitch = 2 * LANES // INNER_ITERS
    row = lax.broadcasted_iota(jnp.int32, (pitch, 2 * LANES), 0)
    column = lax.broadcasted_iota(jnp.int32, (pitch, 2 * LANES), 1)
    powers = [[jnp.where((row == column) & (row < horizon), 1.0, 0.0)] for _ in range(districts)]
    for d in range(districts):
        powers[d].append(jnp.where(row < horizon, weight[d, :pitch, :].astype(F32), 0.0))
    for _ in range(INNER_ITERS - 1):
        for d in range(districts):
            last = powers[d][-1][:, :interface]
            high = last.astype(BF16)
            low = (last - high.astype(F32)).astype(BF16)
            both = mm(jnp.concatenate([high, low], axis=0), weight[d])
            powers[d].append(both[:pitch] + both[pitch:])
    replied = []
    for d in range(districts):
        chosen, added = response(powers[d])
        answer[d] = chosen.astype(BF16)
        answer_sum[d] = added.astype(BF16)
        reply[d] = response(powers[d][1:] + powers[d][:1])[0][:, :LANES].T[:horizon].astype(BF16)

    partners = [
        (step, other)
        for step in range(district_count)
        for other in range(districts)
        if step or other
    ]

    def partner(step, other):
        return {
            "district": lax.rem(my_district + step, district_count),
            "sub": team + lax.rem(role + other, districts),
        }

    reply_copies = []
    for step in range(1, district_count):
        reply_copies.append(
            pltpu.make_async_remote_copy(
                src_ref=reply,
                dst_ref=replies.at[step],
                send_sem=reply_send.at[0],
                recv_sem=reply_recv.at[0],
                device_id={"district": lax.rem(my_district + step, district_count)},
                device_id_type=MESH,
            )
        )
        reply_copies[-1].start()

    moves = relayout_ref[pl.ds(role, 1), :]
    team_rows = districts * rows
    pick = lax.broadcasted_iota(jnp.int32, (team_rows, group), 1) == (
        lax.broadcasted_iota(jnp.int32, (team_rows, group), 0) + team * rows
    )
    pick = jnp.where(pick, 1.0, 0.0).astype(BF16)

    kept = onehot.shape[0] == blocks

    def one_hot(b):
        place = lax.broadcasted_iota(jnp.int32, (block, group), 0) + b * block
        return jnp.where(place == moves, 1.0, 0.0).astype(BF16)

    def choose(b):
        chosen = one_hot(b)
        if kept:
            onehot[b] = chosen
        select[b] = contract(pick, chosen, 1).astype(BF16)

    each(blocks, choose)

    duals[...] = jnp.zeros_like(duals)
    duals[:, :horizon] = capacity_ref[...]
    flow[...] = jnp.zeros_like(flow)
    owned[...] = jnp.zeros_like(owned)
    links[...] = jnp.full_like(links, -window * 4)

    near[me] = tables[role]
    near_all.wait_recv()
    for source in range(sub_count):
        for k in range(LINK_COUNT):
            links[k : k + 1, HALO + source * rows : HALO + (source + 1) * rows] = near[source, k // 2 : k // 2 + 1, k % 2 * rows : (k % 2 + 1) * rows]
        owners[:, source * rows : (source + 1) * rows] = near[source, LINK_COUNT // 2 : LINK_COUNT // 2 + 1, :rows]
    own = owners[...]
    held = lax.broadcasted_iota(jnp.int32, (RESERVOIRS, group), 0)
    match_t[...] = jnp.where(held == own, 1.0, 0.0).astype(BF16)
    held = lax.broadcasted_iota(jnp.int32, (LANES, group), 0)
    hit = (lax.rem(held, RESERVOIRS) == own) & (held < INNER_ITERS * RESERVOIRS)
    owned[0, HALO : HALO + group, :] = jnp.where(hit, 1.0, 0.0).T.astype(BF16)

    def linked(start, width):
        column = lax.broadcasted_iota(jnp.int32, (width, width), 0)
        row = lax.broadcasted_iota(jnp.int32, (width, width), 1)
        table = jnp.where(column == row, 1.0, 0.0)
        for k in range(LINK_COUNT):
            link = links[k : k + 1, pl.ds(start, width)] - (start - HALO)
            table = table - jnp.where(column == link, 1.0 / LINK_COUNT, 0.0)
        return table.T.astype(BF16)

    def build(b):
        start = b * block if isinstance(b, int) else pl.multiple_of(b * block, block)
        table = linked(start, window)
        near_links[b] = table[HALO : HALO + block]
        spread[b] = mm(table[HALO : HALO + block], table).astype(BF16)

    each(blocks, build)
    my_links = near_links.at[team // districts]

    def at_block(b, extra=0, size=block):
        return pl.ds(b * block + extra if isinstance(b, int) else pl.multiple_of(b * block, block) + extra, size)

    lane = lax.broadcasted_iota(jnp.int32, (block, LANES), 1)

    team_window = pl.ds(pl.multiple_of(team * rows, team_rows), window)
    side = lax.broadcasted_iota(jnp.int32, (RESERVOIRS // 2, LANES), 1)

    def halved(values):
        return jnp.where(side < LANES // 2, values[: RESERVOIRS // 2], pltpu.roll(values[RESERVOIRS // 2 :], LANES // 2, 1))

    def whole(values):
        return jnp.concatenate([values, pltpu.roll(values, LANES // 2, 1)], axis=0)

    capacity = halved(duals[...])

    def to_team(source_ref, place_ref, send_sem, recv_sem):
        copies = []
        for other in range(1, districts):
            target = lax.rem(role + other, districts)
            copies.append(
                pltpu.make_async_remote_copy(
                    src_ref=source_ref.at[target],
                    dst_ref=place_ref.at[role],
                    send_sem=send_sem.at[other - 1],
                    recv_sem=recv_sem.at[other - 1],
                    device_id={"sub": team + target},
                    device_id_type=MESH,
                )
            )
            copies[-1].start()
        place_ref[role] = source_ref[role]
        return copies

    def chosen_rows(values):
        chosen = mm(select[0], values(0))
        for b in range(1, blocks):
            chosen = chosen + mm(select[b], values(b))
        return chosen

    for turn in range(1, INNER_ITERS):
        now, later = owned.at[(turn + 1) % 2], owned.at[turn % 2]

        def lengthen(b, turn=turn, now=now, later=later):
            held = now[at_block(b, HALO), :].astype(F32)
            out = mm(spread[b], now[at_block(b, 0, window), :]) - held
            later[at_block(b, HALO), :] = jnp.where(lane < turn * RESERVOIRS, held, out).astype(BF16)

        each(blocks, lengthen)
    owned_all = owned.at[(INNER_ITERS - 1) % 2]

    picked = chosen_rows(lambda b: owned_all[at_block(b, HALO), :])
    local = mm(my_links[...], owned_all[team_window, :])
    factors = jnp.where(lane < LANES // 2, picked, pltpu.roll(local, LANES // 2, 1))
    factors_out[...] = factors.reshape(districts, rows, LANES).astype(BF16)
    returned[...] = halved(mm(match_t[...], owned_all[HALO : HALO + group, :])).astype(BF16)
    factor_copies = to_team(factors_out, factors_in, factors_send, factors_recv)
    return_copies = []
    for index, (step, other) in enumerate(partners):
        return_copies.append(
            pltpu.make_async_remote_copy(
                src_ref=returned,
                dst_ref=returning.at[index],
                send_sem=return_send.at[0],
                recv_sem=return_recv.at[0],
                device_id=partner(step, other),
                device_id_type=MESH,
            )
        )
        return_copies[-1].start()

    flow_all.wait_recv()

    spare = lax.broadcasted_iota(jnp.int32, (rows, LANES), 1) < interface - LANES

    def spread_out(source):
        at = pl.ds(source * rows, rows)
        gathered[at, :LANES] = landed[source, :rows, :]
        tail = unfold(landed[source].astype(F32), rows)
        gathered[at, LANES:] = jnp.where(spare, tail, 0.0).astype(BF16)

    each(sub_count, spread_out)

    def permute(b):
        moved = mm(onehot[b] if kept else one_hot(b), gathered[...])
        base[at_block(b), :] = moved
        flow[at_block(b, HALO), :] = moved.astype(BF16)

    each(blocks, permute)

    total[...] = flow[team_window, :].astype(F32)

    def forward():
        def one(b):
            price = state[at_block(b), :interface].astype(BF16)
            flow[at_block(b, HALO), :] = (base[at_block(b), :] + mm(price, weight[role])).astype(BF16)

        each(blocks, one)
        total[...] += flow[team_window, :].astype(F32)

    def backward(fresh=False):
        def one(b):
            out = mm(spread[b], flow[at_block(b, 0, window), :])
            gain = price_step * out
            state[at_block(b), :] = gain if fresh else state[at_block(b), :] + gain

        each(blocks, one)

    def send_draws(outer):
        drawn = mm(match_t[...], flow[HALO : HALO + group, :])
        draws[outer] = halved(drawn[:, :LANES])
        return start_draws(outer)

    def start_draws(outer):
        copies = []
        for index, (step, other) in enumerate(partners):
            copies.append(
                pltpu.make_async_remote_copy(
                    src_ref=draws.at[outer],
                    dst_ref=arrived.at[outer, index],
                    send_sem=draw_send.at[outer],
                    recv_sem=draw_recv.at[outer],
                    device_id=partner(step, other),
                    device_id_type=MESH,
                )
            )
            copies[-1].start()
        return copies

    def take_draws(outer, copies):
        drawn = draws[outer]
        whole_wait(arrived.at[outer], 0, len(partners), draw_send.at[outer], draw_recv.at[outer], partner(*partners[-1])).wait()
        for index in range(len(partners)):
            drawn = drawn + arrived[outer, index]
        return drawn - capacity

    backward(fresh=True)
    for step in range(1, INNER_ITERS - 1):
        forward()
        backward()
    forward()
    copies = send_draws(0)
    for step in range(INNER_ITERS - 1):
        backward()
        forward()
    backward()
    chosen = chosen_rows(lambda b: state[at_block(b), :].astype(BF16))
    forward()
    high = total[...].astype(BF16)
    low = (total[...] - high.astype(F32)).astype(BF16)
    prices = price_step * (mm(my_links[...], high) + mm(my_links[...], low))
    drawn = mm(match_t[...], flow[HALO : HALO + group, :])
    draws[1] = halved(drawn[:, :LANES])
    for d in range(districts):
        chosen_out[d] = fold(chosen[d * rows : (d + 1) * rows], rows // 2).astype(BF16)
    for d in range(districts):
        prices_out[d] = fold(prices[d * rows : (d + 1) * rows], rows // 2).astype(BF16)
    late_copies = start_draws(1)
    price_copies = to_team(chosen_out, chosen_in, price_send, price_recv)
    dual_copies = to_team(prices_out, prices_in, dual_send, dual_recv)

    drawn = take_draws(0, copies)
    moved = whole(jnp.where(lax.rem(side, LANES // 2) < horizon, drawn * dual_scale, 0.0))
    lanes = lax.broadcasted_iota(jnp.int32, moved.shape, 1)
    moved = jnp.where(lanes < horizon, moved, 0.0)
    half = pltpu.roll(moved, pitch, 1)
    none = jnp.zeros_like(moved)
    steps = jnp.concatenate(
        [
            jnp.concatenate([moved, none], axis=1),
            jnp.concatenate([half, none], axis=1),
            jnp.concatenate([none, moved], axis=1),
            jnp.concatenate([none, half], axis=1),
        ],
        axis=0,
    ).astype(BF16)
    changes = []
    for d in range(districts):
        for_price = mm(steps, answer[d]).astype(BF16)
        for_dual = mm(steps, answer_sum[d]).astype(BF16)
        blank = jnp.zeros_like(for_price)
        changes.append(
            jnp.concatenate(
                [jnp.concatenate([for_price, blank], axis=1), jnp.concatenate([blank, for_dual], axis=1)], axis=0
            )
        )
    for copy in factor_copies:
        copy.wait()
    price_change, dual_change = [], []
    for d in range(districts):
        change = mm(factors_in[d], changes[d])
        price_change.append(change[:, : 2 * LANES])
        dual_change.append(change[:, 2 * LANES :])

    across = partner(*partners[-1])
    whole_wait(returning, 0, len(partners), return_send.at[0], return_recv.at[0], across).wait()
    whole_wait(replies, 1, district_count - 1, reply_send.at[0], reply_recv.at[0], across).wait()
    heard = [whole(returned[...].astype(F32))] + [whole(returning[index].astype(F32)) for index in range(len(partners))]
    returns = mm(jnp.concatenate(heard, axis=0)[:, : LANES // 2].astype(BF16), steps).astype(BF16)
    late = contract(returns[:RESERVOIRS], reply[role], 1)
    for index, (step, other) in enumerate(partners):
        at = slice((index + 1) * RESERVOIRS, (index + 2) * RESERVOIRS)
        source = lax.rem(role + districts - other, districts)
        late = late + contract(returns[at], replies[step, source] if step else reply[source], 1)

    for copy in price_copies:
        copy.wait()
    for d in range(districts):
        price = unfolded(chosen_in[d].astype(F32), rows)[:, :interface] + price_change[d][:, :interface]
        plan_ref[d] = plan_ref[d] - mm(price.astype(BF16), inner[d])
    for copy in dual_copies:
        copy.wait()
    for d in range(districts):
        prices_ref[d] = unfolded(prices_in[d].astype(F32), rows)[:, :interface] + dual_change[d][:, :interface]
    drawn = whole(take_draws(1, late_copies))
    duals_ref[...] = moved[:, :horizon] + (drawn[:, :horizon] + late) * dual_scale
    near_all.wait_send()
    flow_all.wait_send()


def handover(plan_ref, prices_ref, duals_ref, plan_out, prices_out, duals_out, sem):
    copies = [
        pltpu.make_async_copy(source, target, sem.at[index])
        for index, (source, target) in enumerate(
            ((plan_ref, plan_out), (prices_ref, prices_out), (duals_ref, duals_out))
        )
    ]
    for copy in copies:
        copy.start()
    for copy in copies:
        copy.wait()


def on_device(cost_terms, neighbours, relayout, ownership, capacity, coupling, solve_factor):
    districts, rows, unknowns = cost_terms.shape
    interface = coupling.shape[2]
    group = relayout.shape[1]
    sub_count = lax.axis_size("sub")
    district_count = lax.axis_size("district")
    load_count = districts * district_count * group // (2 * RESERVOIRS)
    dual_scale = reserve_step / math.sqrt(load_count)
    near = neighbours.transpose(0, 2, 1).reshape(districts * LINK_COUNT, rows)
    coupling = coupling.transpose(0, 2, 1)
    block = districts * rows
    blocks = group // block
    window = block + 2 * HALO
    vmem = pl.BlockSpec(memory_space=pltpu.VMEM)
    hbm = pl.BlockSpec(memory_space=pl.ANY)
    dma = pltpu.SemaphoreType.DMA
    results = pl.pallas_call(
        functools.partial(kernel, dual_scale),
        name="districts",
        out_shape=(
            jax.ShapeDtypeStruct((districts, rows, unknowns), F32),
            jax.ShapeDtypeStruct((districts, rows, interface), F32),
            jax.ShapeDtypeStruct(capacity.shape, F32),
        ),
        in_specs=[pl.BlockSpec(memory_space=pltpu.HBM)] * 7,
        out_specs=(vmem, vmem, vmem),
        scratch_shapes=[
            pltpu.VMEM(cost_terms.shape, BF16),
            pltpu.VMEM(near.shape, jnp.int32),
            pltpu.VMEM(ownership.shape, jnp.int32),
            pltpu.VMEM(relayout.shape, jnp.int32),
            pltpu.VMEM(capacity.shape, F32),
            pltpu.VMEM(coupling.shape, BF16),
            pltpu.VMEM(solve_factor.shape, BF16),
            pltpu.VMEM((districts, LINK_COUNT, LANES), jnp.int32),
            pltpu.VMEM((sub_count, LINK_COUNT, LANES), jnp.int32),
            pltpu.VMEM((LINK_COUNT, group + 2 * HALO), jnp.int32),
            pltpu.VMEM((1, group), jnp.int32),
            pltpu.VMEM((rows, 2 * LANES), F32),
            pltpu.VMEM((districts, rows + rows // 2, LANES), BF16),
            pltpu.VMEM((sub_count, rows + rows // 2, LANES), BF16),
            pltpu.VMEM((group, 2 * LANES), BF16),
            pltpu.VMEM((group, 2 * LANES), F32),
            pltpu.VMEM((group, 2 * LANES), F32),
            pltpu.VMEM((group + 2 * HALO, 2 * LANES), BF16),
            pltpu.VMEM((window, 2 * LANES), F32),
            pltpu.VMEM((blocks, block, window), BF16),
            pltpu.VMEM((districts, interface, unknowns), BF16),
            pltpu.VMEM((districts, interface, 2 * LANES), BF16),
            pltpu.VMEM((districts, 2 * LANES, 2 * LANES), BF16),
            pltpu.VMEM((districts, 2 * LANES, 2 * LANES), BF16),
            pltpu.VMEM((districts, capacity.shape[1], 2 * LANES), BF16),
            pltpu.VMEM((district_count, districts, capacity.shape[1], 2 * LANES), BF16),
            pltpu.VMEM((RESERVOIRS, group), BF16),
            pltpu.VMEM((2, group + 2 * HALO, LANES), BF16),
            pltpu.VMEM((blocks if group <= 1024 else 1, block, group), BF16),
            pltpu.VMEM((blocks, block, block), BF16),
            pltpu.VMEM((blocks, block, window), BF16),
            pltpu.VMEM((districts, rows, LANES), BF16),
            pltpu.VMEM((districts, rows, LANES), BF16),
            pltpu.VMEM((districts, rows + rows // 2, LANES), BF16),
            pltpu.VMEM((districts, rows + rows // 2, LANES), BF16),
            pltpu.VMEM((districts, rows + rows // 2, LANES), BF16),
            pltpu.VMEM((districts, rows + rows // 2, LANES), BF16),
            pltpu.VMEM((RESERVOIRS, LANES), F32),
            pltpu.VMEM((OUTER_ITERS, RESERVOIRS // 2, LANES), F32),
            pltpu.VMEM((OUTER_ITERS, district_count * districts, RESERVOIRS // 2, LANES), F32),
            pltpu.VMEM((RESERVOIRS // 2, LANES), BF16),
            pltpu.VMEM((district_count * districts, RESERVOIRS // 2, LANES), BF16),
            dma((2 * districts + 5,)),
            dma((1,)),
            dma((1,)),
            dma((1,)),
            dma((1,)),
            dma((OUTER_ITERS,)),
            dma((OUTER_ITERS,)),
            dma((1,)),
            dma((1,)),
            dma((1,)),
            dma((1,)),
            dma((districts - 1,)),
            dma((districts - 1,)),
            dma((districts - 1,)),
            dma((districts - 1,)),
            dma((districts - 1,)),
            dma((districts - 1,)),
        ],
        compiler_params=pltpu.CompilerParams(
            collective_id=0, has_side_effects=True, vmem_limit_bytes=(20 if group <= 1024 else 60) * 1024 * 1024
        ),
    )(*[pltpu.with_memory_space_constraint(value, pltpu.HBM) for value in (cost_terms, near, ownership, relayout, capacity, coupling, solve_factor)])
    return pl.pallas_call(
        handover,
        name="handover",
        out_shape=tuple(jax.ShapeDtypeStruct(value.shape, value.dtype) for value in results),
        in_specs=[hbm] * 3,
        out_specs=(hbm,) * 3,
        scratch_shapes=[dma((3,))],
        compiler_params=pltpu.CompilerParams(vmem_limit_bytes=4 * 1024 * 1024),
    )(*results)


def solution(mesh):
    placed = (
        P("district", "sub", None),
        P("district", "sub", None),
        P("district", None),
        P("district", "sub"),
        P(),
        P("district", None, None),
        P("district", None, None),
    )
    return jax.shard_map(
        on_device,
        mesh=mesh,
        in_specs=placed,
        out_specs=(P("district", "sub", None), P("district", "sub", None), P()),
        check_vma=False,
    )
```

```python
import functools
import math

import jax
import jax.numpy as jnp
from jax import lax
from jax.experimental import pallas as pl
from jax.experimental.pallas import tpu as pltpu
from jax.sharding import PartitionSpec as P

REACH_SPAN = 16
LINK_COUNT = 4
RESERVOIRS = 16
OUTER_ITERS = 2
INNER_ITERS = 4
HALO = 2 * REACH_SPAN
LANES = 128

price_step = 0.3
reserve_step = 1.0

F32 = jnp.float32
BF16 = jnp.bfloat16
MESH = pl.DeviceIdType.MESH


def each(count, body):
    if count <= 8:
        for index in range(count):
            body(index)
    else:
        lax.fori_loop(0, count, lambda index, carry: (body(index), carry)[1], 0)


def mm(a, b):
    return jnp.dot(a, b, preferred_element_type=F32)


def contract(a, b, dim):
    return lax.dot_general(a, b, (((dim,), (dim,)), ((), ())), preferred_element_type=F32)


def fold(wide, half):
    tail = wide[:, LANES:]
    lane = lax.broadcasted_iota(jnp.int32, (half, LANES), 1)
    folded = jnp.where(lane < LANES // 2, tail[:half], pltpu.roll(tail[half:], LANES // 2, 1))
    return jnp.concatenate([wide[:, :LANES], folded], axis=0)


def unfold(folded, rows):
    tail = folded[rows:]
    return jnp.concatenate([tail, pltpu.roll(tail, LANES // 2, 1)], axis=0)


def unfolded(folded, rows):
    return jnp.concatenate([folded[:rows], unfold(folded, rows)], axis=1)


def response(powers):
    shift, summed = [], []
    for i in range(INNER_ITERS):
        chosen, added = 0.0, 0.0
        for j in range(i, INNER_ITERS):
            scale = price_step ** j
            chosen = chosen + scale * math.comb(INNER_ITERS - 1, i) * math.comb(INNER_ITERS - 1 - i, j - i) * powers[j]
            weight = sum(math.comb(k, i) * math.comb(k - i, j - i) for k in range(j, INNER_ITERS))
            added = added + price_step * scale * weight * powers[j + 1]
        shift.append(chosen)
        summed.append(added)
    return jnp.concatenate(shift, axis=0), jnp.concatenate(summed, axis=0)


def whole_wait(place_ref, start, count, send_sem, recv_sem, device):
    places = place_ref.at[pl.ds(start, count)]
    return pltpu.make_async_remote_copy(
        src_ref=places, dst_ref=places, send_sem=send_sem, recv_sem=recv_sem, device_id=device, device_id_type=MESH
    )


def target_of(index, me, count, width):
    place, turn = me // width, lax.rem(me, width)
    pairs = count // width
    if index >= count - width:
        return place * width + lax.rem(turn + 1 + index - (count - width), width)
    slot = index // width
    low = 1 - jnp.minimum(place // (pairs // 2), 1)
    climb = slot + jnp.minimum(jnp.maximum(slot - place + 1, 0), 1)
    fall = pairs - 1 - slot
    fall = fall - jnp.minimum(jnp.maximum(place - fall + 1, 0), 1)
    return (low * fall + (1 - low) * climb) * width + lax.rem(turn + 1 + index % width, width)


def chunks_of(unknowns):
    return 1 if unknowns % 128 == 0 else 1


def kernel(
    dual_scale, costs_hbm, near_hbm, owner_hbm, relayout_hbm, capacity_hbm, coupling_hbm, factor_hbm,
    plan_ref, prices_ref, duals_ref,
    costs_ref, near_ref, owner_ref, relayout_ref, capacity_ref, coupling, factor, tables, near, links, owners, wide_first, first, landed, gathered, base, state, flow, total, spread, inner, weight, answer, reply, replies,
    match_t, owned, onehot, select, near_links, factors_out, factors_in, chosen_out, chosen_in, prices_out, prices_in, duals, draws, arrived, returned, returning,
    local_sem, near_send, near_recv, flow_send, flow_recv, draw_send, draw_recv, reply_send, reply_recv, return_send, return_recv,
    factors_send, factors_recv, price_send, price_recv, dual_send, dual_recv,
):
    districts, rows, unknowns = costs_ref.shape
    interface = coupling.shape[1]
    horizon = capacity_ref.shape[1]
    group = relayout_ref.shape[1]
    sub_count = lax.axis_size("sub")
    district_count = lax.axis_size("district")
    me = lax.axis_index("sub")
    role = lax.rem(me, districts)
    team = me // districts * districts
    my_district = lax.axis_index("district")
    block = districts * rows
    window = block + 2 * HALO
    blocks = group // block
    half_count = sub_count // 2
    front = 1 - jnp.minimum(me // half_count, 1)

    def slot_of(source, place):
        far = jnp.minimum(place // half_count, 1)
        return lax.rem(source + far * half_count, sub_count)

    chunks = chunks_of(unknowns)
    chunk = unknowns // chunks
    small_loads = [
        pltpu.make_async_copy(source, target, local_sem.at[index])
        for index, (source, target) in enumerate(
            (
                (near_hbm, near_ref),
                (owner_hbm, owner_ref),
                (relayout_hbm, relayout_ref),
                (capacity_hbm, capacity_ref),
            )
        )
    ]
    costs_load = pltpu.make_async_copy(costs_hbm, costs_ref, local_sem.at[4])
    costs_load.start()
    loads = []
    for turn in range(districts):
        d = lax.rem(role + 1 + turn, districts)
        loads.append([])
        for part in range(chunks):
            at = pl.ds(part * chunk, chunk)
            loads[-1].append(pltpu.make_async_copy(factor_hbm.at[d, at], factor.at[d, at], local_sem.at[5 + turn * (chunks + 1) + part]))
        loads[-1].append(pltpu.make_async_copy(coupling_hbm.at[d], coupling.at[d], local_sem.at[5 + turn * (chunks + 1) + chunks]))
        for load in loads[-1]:
            load.start()
        if turn == 0:
            for load in small_loads:
                load.start()

    barrier = pltpu.get_barrier_semaphore()
    for step in range(1, sub_count):
        pl.semaphore_signal(
            barrier, inc=1, device_id={"sub": lax.rem(me + step, sub_count)}, device_id_type=MESH
        )
    for step in range(1, district_count):
        for other in range(districts):
            pl.semaphore_signal(
                barrier,
                inc=1,
                device_id={
                    "district": lax.rem(my_district + step, district_count),
                    "sub": team + lax.rem(role + other, districts),
                },
                device_id_type=MESH,
            )

    beside = {"sub": lax.rem(me + 1, sub_count)}
    near_all = whole_wait(near, 0, sub_count - 1, near_send.at[0], near_recv.at[0], beside)
    flow_all = whole_wait(landed, 0, sub_count - 1, flow_send.at[0], flow_recv.at[0], beside)
    flow_own = whole_wait(landed, 0, half_count - 1, flow_send.at[0], flow_recv.at[0], beside)
    flow_far = whole_wait(landed, 0, half_count, flow_send.at[0], flow_recv.at[1], beside)
    def send_to(index, source_ref, place_ref, send_sem, recv_sem):
        pltpu.make_async_remote_copy(
            src_ref=source_ref,
            dst_ref=place_ref,
            send_sem=send_sem,
            recv_sem=recv_sem,
            device_id={"sub": target_of(index, me, sub_count, districts)},
            device_id_type=MESH,
        ).start()

    def send_tables():
        pl.semaphore_wait(barrier, sub_count - 1 + (district_count - 1) * districts)
        for index in range(sub_count - 1):
            target = target_of(index, me, sub_count, districts)
            send_to(index, tables.at[lax.rem(target, districts)], near.at[me], near_send.at[0], near_recv.at[0])

    def send_flows(turn):
        for index in range(sub_count - 1):
            if index % districts == turn:
                target = target_of(index, me, sub_count, districts)
                send_to(index, first.at[lax.rem(target, districts)], landed.at[slot_of(me, target)], flow_send.at[0], flow_recv.at[1 if index < half_count else 0])

    def compute_first(turn):
        d = lax.rem(role + 1 + turn, districts)
        first_plan = jnp.zeros((rows, unknowns), F32)
        for part in range(chunks):
            loads[turn][part].wait()
            at = slice(part * chunk, (part + 1) * chunk)
            product = mm(costs_ref[d, :, at], factor[d, at, :])
            first_plan = product if part == 0 else first_plan + product
        loads[turn][chunks].wait()
        first_plan = -first_plan
        plan_ref[d] = first_plan
        wide_first[:, :interface] = contract(first_plan.astype(BF16), coupling[d], 1)
        first[d] = fold(wide_first[...], rows // 2).astype(BF16)

    costs_load.wait()
    for load in small_loads:
        load.wait()
    for d in range(districts):
        for k in range(LINK_COUNT):
            tables[d, k // 2 : k // 2 + 1, k % 2 * rows : (k % 2 + 1) * rows] = near_ref[d * LINK_COUNT + k : d * LINK_COUNT + k + 1, :]
        tables[d, LINK_COUNT // 2 : LINK_COUNT // 2 + 1, :rows] = owner_ref[d : d + 1, :]
    compute_first(0)
    send_tables()
    send_flows(0)
    for turn in range(1, districts):
        compute_first(turn)
        send_flows(turn)

    landed[slot_of(me, me)] = first[role]
    for d in range(districts):
        inner[d] = mm(coupling[d], factor[d]).astype(BF16)
        weight[d] = jnp.zeros_like(weight[d])
        weight[d, :, :interface] = (-contract(inner[d], coupling[d], 1)).astype(BF16)

    span = 2 * LANES
    pitch = span // INNER_ITERS
    row = lax.broadcasted_iota(jnp.int32, (pitch, 2 * LANES), 0)
    column = lax.broadcasted_iota(jnp.int32, (pitch, 2 * LANES), 1)
    powers = [[jnp.where((row == column) & (row < horizon), 1.0, 0.0)] for _ in range(districts)]
    for d in range(districts):
        powers[d].append(jnp.where(row < horizon, weight[d, :pitch, :].astype(F32), 0.0))
    for _ in range(INNER_ITERS - 1):
        for d in range(districts):
            last = powers[d][-1][:, :interface]
            high = last.astype(BF16)
            low = (last - high.astype(F32)).astype(BF16)
            both = mm(jnp.concatenate([high, low], axis=0), weight[d])
            powers[d].append(both[:pitch] + both[pitch:])
    replied = []
    for d in range(districts):
        chosen, added = response(powers[d])
        answer[:, 2 * d * span : (2 * d + 1) * span] = chosen.astype(BF16)
        answer[:, (2 * d + 1) * span : (2 * d + 2) * span] = added.astype(BF16)
        reply[d] = response(powers[d][1:] + powers[d][:1])[0][:, :LANES].T[:horizon].astype(BF16)

    partners = [
        (step, other)
        for step in range(district_count)
        for other in range(districts)
        if step or other
    ]

    def partner(step, other):
        return {
            "district": lax.rem(my_district + step, district_count),
            "sub": team + lax.rem(role + other, districts),
        }

    reply_copies = []
    for step in range(1, district_count):
        reply_copies.append(
            pltpu.make_async_remote_copy(
                src_ref=reply,
                dst_ref=replies.at[step],
                send_sem=reply_send.at[0],
                recv_sem=reply_recv.at[0],
                device_id={"district": lax.rem(my_district + step, district_count)},
                device_id_type=MESH,
            )
        )
        reply_copies[-1].start()

    moves = relayout_ref[pl.ds(role, 1), :]
    moves = jnp.where(front == 1, moves, jnp.concatenate([moves[:, group // 2 :], moves[:, : group // 2]], axis=1))
    team_rows = districts * rows
    pick = lax.broadcasted_iota(jnp.int32, (team_rows, group), 1) == (
        lax.broadcasted_iota(jnp.int32, (team_rows, group), 0) + team * rows - (1 - front) * (group // 2)
    )
    pick = jnp.where(pick, 1.0, 0.0).astype(BF16)

    kept = onehot.shape[0] == blocks

    def one_hot(b):
        place = lax.broadcasted_iota(jnp.int32, (block, group), 0) + b * block
        return jnp.where(place == moves, 1.0, 0.0).astype(BF16)

    def choose(b):
        chosen = one_hot(b)
        if kept:
            onehot[b] = chosen
        select[b] = contract(pick, chosen, 1).astype(BF16)

    each(blocks, choose)

    duals[...] = jnp.zeros_like(duals)
    duals[:, :horizon] = capacity_ref[...]
    flow[...] = jnp.zeros_like(flow)
    owned[...] = jnp.zeros_like(owned)
    links[...] = jnp.full_like(links, -window * 4)

    near[me] = tables[role]
    near_all.wait_recv()
    for source in range(sub_count):
        for k in range(LINK_COUNT):
            links[k : k + 1, HALO + source * rows : HALO + (source + 1) * rows] = near[source, k // 2 : k // 2 + 1, k % 2 * rows : (k % 2 + 1) * rows]
        owners[:, source * rows : (source + 1) * rows] = near[source, LINK_COUNT // 2 : LINK_COUNT // 2 + 1, :rows]
    own = owners[...]
    held = lax.broadcasted_iota(jnp.int32, (RESERVOIRS, group), 0)
    match_t[...] = jnp.where(held == own, 1.0, 0.0).astype(BF16)
    held = lax.broadcasted_iota(jnp.int32, (LANES, group), 0)
    hit = (lax.rem(held, RESERVOIRS) == own) & (held < INNER_ITERS * RESERVOIRS)
    owned[0, HALO : HALO + group, :] = jnp.where(hit, 1.0, 0.0).T.astype(BF16)

    def linked(start, width):
        column = lax.broadcasted_iota(jnp.int32, (width, width), 0)
        row = lax.broadcasted_iota(jnp.int32, (width, width), 1)
        table = jnp.where(column == row, 1.0, 0.0)
        for k in range(LINK_COUNT):
            link = links[k : k + 1, pl.ds(start, width)] - (start - HALO)
            table = table - jnp.where(column == link, 1.0 / LINK_COUNT, 0.0)
        return table.T.astype(BF16)

    def build(b):
        start = b * block if isinstance(b, int) else pl.multiple_of(b * block, block)
        table = linked(start, window)
        near_links[b] = table[HALO : HALO + block]
        spread[b] = mm(table[HALO : HALO + block], table).astype(BF16)

    each(blocks, build)
    my_links = near_links.at[team // districts]

    def at_block(b, extra=0, size=block):
        return pl.ds(b * block + extra if isinstance(b, int) else pl.multiple_of(b * block, block) + extra, size)

    lane = lax.broadcasted_iota(jnp.int32, (block, LANES), 1)

    team_window = pl.ds(pl.multiple_of(team * rows, team_rows), window)
    side = lax.broadcasted_iota(jnp.int32, (RESERVOIRS // 2, LANES), 1)

    def halved(values):
        return jnp.where(side < LANES // 2, values[: RESERVOIRS // 2], pltpu.roll(values[RESERVOIRS // 2 :], LANES // 2, 1))

    def whole(values):
        return jnp.concatenate([values, pltpu.roll(values, LANES // 2, 1)], axis=0)

    capacity = halved(duals[...])

    def to_team(source_ref, place_ref, send_sem, recv_sem):
        copies = []
        for other in range(1, districts):
            target = lax.rem(role + other, districts)
            copies.append(
                pltpu.make_async_remote_copy(
                    src_ref=source_ref.at[target],
                    dst_ref=place_ref.at[role],
                    send_sem=send_sem.at[other - 1],
                    recv_sem=recv_sem.at[other - 1],
                    device_id={"sub": team + target},
                    device_id_type=MESH,
                )
            )
            copies[-1].start()
        place_ref[role] = source_ref[role]
        return copies

    def chosen_rows(values):
        chosen = mm(select[0], values(0))
        for b in range(1, blocks):
            chosen = chosen + mm(select[b], values(b))
        return chosen

    for turn in range(1, INNER_ITERS):
        now, later = owned.at[(turn + 1) % 2], owned.at[turn % 2]

        def lengthen(b, turn=turn, now=now, later=later):
            held = now[at_block(b, HALO), :].astype(F32)
            out = mm(spread[b], now[at_block(b, 0, window), :]) - held
            later[at_block(b, HALO), :] = jnp.where(lane < turn * RESERVOIRS, held, out).astype(BF16)

        each(blocks, lengthen)
    owned_all = owned.at[(INNER_ITERS - 1) % 2]

    picked = chosen_rows(lambda b: owned_all[at_block(b, HALO), :])
    local = mm(my_links[...], owned_all[team_window, :])
    factors = jnp.where(lane < LANES // 2, picked, pltpu.roll(local, LANES // 2, 1))
    factors_out[...] = factors.reshape(districts, rows, LANES).astype(BF16)
    returned[...] = halved(mm(match_t[...], owned_all[HALO : HALO + group, :])).astype(BF16)
    factor_copies = to_team(factors_out, factors_in, factors_send, factors_recv)
    return_copies = []
    for index, (step, other) in enumerate(partners):
        return_copies.append(
            pltpu.make_async_remote_copy(
                src_ref=returned,
                dst_ref=returning.at[index],
                send_sem=return_send.at[0],
                recv_sem=return_recv.at[0],
                device_id=partner(step, other),
                device_id_type=MESH,
            )
        )
        return_copies[-1].start()


    spare = lax.broadcasted_iota(jnp.int32, (rows, LANES), 1) < interface - LANES

    def spread_out(source):
        at = pl.ds(source * rows, rows)
        gathered[at, :LANES] = landed[source, :rows, :]
        tail = unfold(landed[source].astype(F32), rows)
        gathered[at, LANES:] = jnp.where(spare, tail, 0.0).astype(BF16)

    middle = group // 2

    def permute(b):
        chosen = onehot[b] if kept else one_hot(b)
        base[at_block(b), :] = mm(chosen[:, :middle], gathered[:middle, :])

    def permute_far(b):
        chosen = onehot[b] if kept else one_hot(b)
        moved = base[at_block(b), :] + mm(chosen[:, middle:], gathered[middle:, :])
        base[at_block(b), :] = moved
        flow[at_block(b, HALO), :] = moved.astype(BF16)

    flow_own.wait_recv()
    each(half_count, spread_out)
    each(blocks, permute)
    flow_far.wait_recv()
    each(half_count, lambda source: spread_out(source + half_count))
    each(blocks, permute_far)

    total[...] = flow[team_window, :].astype(F32)

    def forward():
        def one(b):
            price = state[at_block(b), :interface].astype(BF16)
            flow[at_block(b, HALO), :] = (base[at_block(b), :] + mm(price, weight[role])).astype(BF16)

        each(blocks, one)
        total[...] += flow[team_window, :].astype(F32)

    def backward(fresh=False):
        def one(b):
            out = mm(spread[b], flow[at_block(b, 0, window), :])
            gain = price_step * out
            state[at_block(b), :] = gain if fresh else state[at_block(b), :] + gain

        each(blocks, one)

    def start_draws(outer):
        copies = []
        for index, (step, other) in enumerate(partners):
            copies.append(
                pltpu.make_async_remote_copy(
                    src_ref=draws.at[outer],
                    dst_ref=arrived.at[outer, index],
                    send_sem=draw_send.at[outer],
                    recv_sem=draw_recv.at[outer],
                    device_id=partner(step, other),
                    device_id_type=MESH,
                )
            )
            copies[-1].start()
        return copies

    def take_draws(outer, copies):
        drawn = draws[outer]
        whole_wait(arrived.at[outer], 0, len(partners), draw_send.at[outer], draw_recv.at[outer], partner(*partners[-1])).wait()
        for index in range(len(partners)):
            drawn = drawn + arrived[outer, index]
        return drawn - capacity

    backward(fresh=True)
    for step in range(1, INNER_ITERS - 1):
        forward()
        backward()
    forward()
    drawn = mm(match_t[...], flow[HALO : HALO + group, :])
    draws[0] = halved(drawn[:, :LANES])
    copies = start_draws(0)
    for step in range(INNER_ITERS - 1):
        backward()
        forward()
    backward()
    forward()
    drawn = mm(match_t[...], flow[HALO : HALO + group, :])
    draws[1] = halved(drawn[:, :LANES])
    late_copies = start_draws(1)
    chosen = chosen_rows(lambda b: state[at_block(b), :].astype(BF16))
    for d in range(districts):
        chosen_out[d] = fold(chosen[d * rows : (d + 1) * rows], rows // 2).astype(BF16)
    price_copies = to_team(chosen_out, chosen_in, price_send, price_recv)
    high = total[...].astype(BF16)
    low = (total[...] - high.astype(F32)).astype(BF16)
    prices = price_step * (mm(my_links[...], high) + mm(my_links[...], low))
    for d in range(districts):
        prices_out[d] = fold(prices[d * rows : (d + 1) * rows], rows // 2).astype(BF16)
    dual_copies = to_team(prices_out, prices_in, dual_send, dual_recv)

    for copy in factor_copies:
        copy.wait()
    across = partner(*partners[-1])
    whole_wait(returning, 0, len(partners), return_send.at[0], return_recv.at[0], across).wait()
    whole_wait(replies, 1, district_count - 1, reply_send.at[0], reply_recv.at[0], across).wait()
    heard = [whole(returned[...].astype(F32))] + [whole(returning[index].astype(F32)) for index in range(len(partners))]
    heard = jnp.concatenate(heard, axis=0)[:, : LANES // 2].astype(BF16)

    drawn = take_draws(0, copies)
    moved = whole(jnp.where(lax.rem(side, LANES // 2) < horizon, drawn * dual_scale, 0.0))
    lanes = lax.broadcasted_iota(jnp.int32, moved.shape, 1)
    moved = jnp.where(lanes < horizon, moved, 0.0)
    half = pltpu.roll(moved, pitch, 1)
    none = jnp.zeros_like(moved)
    steps = jnp.concatenate(
        [
            jnp.concatenate([moved, none], axis=1),
            jnp.concatenate([half, none], axis=1),
            jnp.concatenate([none, moved], axis=1),
            jnp.concatenate([none, half], axis=1),
        ],
        axis=0,
    ).astype(BF16)
    turned = mm(steps, answer[...]).astype(BF16)
    returns = mm(heard, steps).astype(BF16)
    changes = []
    for d in range(districts):
        fit = factors_in[d]
        changes.append(
            (
                mm(fit[:, : LANES // 2], turned[:, 2 * d * span : (2 * d + 1) * span])[:, :interface],
                mm(fit[:, LANES // 2 :], turned[:, (2 * d + 1) * span : (2 * d + 2) * span])[:, :interface],
            )
        )
    late = contract(returns[:RESERVOIRS], reply[role], 1)
    for index, (step, other) in enumerate(partners):
        at = slice((index + 1) * RESERVOIRS, (index + 2) * RESERVOIRS)
        source = lax.rem(role + districts - other, districts)
        late = late + contract(returns[at], replies[step, source] if step else reply[source], 1)
    for copy in price_copies:
        copy.wait()
    for d in range(districts):
        price = unfolded(chosen_in[d].astype(F32), rows)[:, :interface] + changes[d][0]
        plan_ref[d] = plan_ref[d] - mm(price.astype(BF16), inner[d])
    for copy in dual_copies:
        copy.wait()
    for d in range(districts):
        prices_ref[d] = unfolded(prices_in[d].astype(F32), rows)[:, :interface] + changes[d][1]
    drawn = whole(take_draws(1, late_copies))
    duals_ref[...] = moved[:, :horizon] + (drawn[:, :horizon] + late) * dual_scale
    near_all.wait_send()
    flow_all.wait_send()


def handover(plan_ref, prices_ref, duals_ref, plan_out, prices_out, duals_out, sem):
    copies = [
        pltpu.make_async_copy(source, target, sem.at[index])
        for index, (source, target) in enumerate(
            ((plan_ref, plan_out), (prices_ref, prices_out), (duals_ref, duals_out))
        )
    ]
    for copy in copies:
        copy.start()
    for copy in copies:
        copy.wait()


def on_device(cost_terms, neighbours, relayout, ownership, capacity, coupling, solve_factor):
    districts, rows, unknowns = cost_terms.shape
    interface = coupling.shape[2]
    group = relayout.shape[1]
    sub_count = lax.axis_size("sub")
    district_count = lax.axis_size("district")
    load_count = districts * district_count * group // (2 * RESERVOIRS)
    dual_scale = reserve_step / math.sqrt(load_count)
    near = neighbours.transpose(0, 2, 1).reshape(districts * LINK_COUNT, rows)
    coupling = coupling.transpose(0, 2, 1)
    block = districts * rows
    blocks = group // block
    window = block + 2 * HALO
    vmem = pl.BlockSpec(memory_space=pltpu.VMEM)
    hbm = pl.BlockSpec(memory_space=pl.ANY)
    dma = pltpu.SemaphoreType.DMA
    results = pl.pallas_call(
        functools.partial(kernel, dual_scale),
        name="districts",
        out_shape=(
            jax.ShapeDtypeStruct((districts, rows, unknowns), F32),
            jax.ShapeDtypeStruct((districts, rows, interface), F32),
            jax.ShapeDtypeStruct(capacity.shape, F32),
        ),
        in_specs=[pl.BlockSpec(memory_space=pltpu.HBM)] * 7,
        out_specs=(vmem, vmem, vmem),
        scratch_shapes=[
            pltpu.VMEM(cost_terms.shape, BF16),
            pltpu.VMEM(near.shape, jnp.int32),
            pltpu.VMEM(ownership.shape, jnp.int32),
            pltpu.VMEM(relayout.shape, jnp.int32),
            pltpu.VMEM(capacity.shape, F32),
            pltpu.VMEM(coupling.shape, BF16),
            pltpu.VMEM(solve_factor.shape, BF16),
            pltpu.VMEM((districts, LINK_COUNT, LANES), jnp.int32),
            pltpu.VMEM((sub_count, LINK_COUNT, LANES), jnp.int32),
            pltpu.VMEM((LINK_COUNT, group + 2 * HALO), jnp.int32),
            pltpu.VMEM((1, group), jnp.int32),
            pltpu.VMEM((rows, 2 * LANES), F32),
            pltpu.VMEM((districts, rows + rows // 2, LANES), BF16),
            pltpu.VMEM((sub_count, rows + rows // 2, LANES), BF16),
            pltpu.VMEM((group, 2 * LANES), BF16),
            pltpu.VMEM((group, 2 * LANES), F32),
            pltpu.VMEM((group, 2 * LANES), F32),
            pltpu.VMEM((group + 2 * HALO, 2 * LANES), BF16),
            pltpu.VMEM((window, 2 * LANES), F32),
            pltpu.VMEM((blocks, block, window), BF16),
            pltpu.VMEM((districts, interface, unknowns), BF16),
            pltpu.VMEM((districts, interface, 2 * LANES), BF16),
            pltpu.VMEM((2 * LANES, 4 * LANES * districts), BF16),
            pltpu.VMEM((districts, capacity.shape[1], 2 * LANES), BF16),
            pltpu.VMEM((district_count, districts, capacity.shape[1], 2 * LANES), BF16),
            pltpu.VMEM((RESERVOIRS, group), BF16),
            pltpu.VMEM((2, group + 2 * HALO, LANES), BF16),
            pltpu.VMEM((blocks if group <= 1024 else 1, block, group), BF16),
            pltpu.VMEM((blocks, block, block), BF16),
            pltpu.VMEM((blocks, block, window), BF16),
            pltpu.VMEM((districts, rows, LANES), BF16),
            pltpu.VMEM((districts, rows, LANES), BF16),
            pltpu.VMEM((districts, rows + rows // 2, LANES), BF16),
            pltpu.VMEM((districts, rows + rows // 2, LANES), BF16),
            pltpu.VMEM((districts, rows + rows // 2, LANES), BF16),
            pltpu.VMEM((districts, rows + rows // 2, LANES), BF16),
            pltpu.VMEM((RESERVOIRS, LANES), F32),
            pltpu.VMEM((OUTER_ITERS, RESERVOIRS // 2, LANES), F32),
            pltpu.VMEM((OUTER_ITERS, district_count * districts, RESERVOIRS // 2, LANES), F32),
            pltpu.VMEM((RESERVOIRS // 2, LANES), BF16),
            pltpu.VMEM((district_count * districts, RESERVOIRS // 2, LANES), BF16),
            dma((districts * (chunks_of(unknowns) + 1) + 5,)),
            dma((1,)),
            dma((1,)),
            dma((1,)),
            dma((2,)),
            dma((OUTER_ITERS,)),
            dma((OUTER_ITERS,)),
            dma((1,)),
            dma((1,)),
            dma((1,)),
            dma((1,)),
            dma((districts - 1,)),
            dma((districts - 1,)),
            dma((districts - 1,)),
            dma((districts - 1,)),
            dma((districts - 1,)),
            dma((districts - 1,)),
        ],
        compiler_params=pltpu.CompilerParams(
            collective_id=0, has_side_effects=True, vmem_limit_bytes=(20 if group <= 1024 else 60) * 1024 * 1024
        ),
    )(*[pltpu.with_memory_space_constraint(value, pltpu.HBM) for value in (cost_terms, near, ownership, relayout, capacity, coupling, solve_factor)])
    return pl.pallas_call(
        handover,
        name="handover",
        out_shape=tuple(jax.ShapeDtypeStruct(value.shape, value.dtype) for value in results),
        in_specs=[hbm] * 3,
        out_specs=(hbm,) * 3,
        scratch_shapes=[dma((3,))],
        compiler_params=pltpu.CompilerParams(vmem_limit_bytes=4 * 1024 * 1024),
    )(*results)


def solution(mesh):
    placed = (
        P("district", "sub", None),
        P("district", "sub", None),
        P("district", None),
        P("district", "sub"),
        P(),
        P("district", None, None),
        P("district", None, None),
    )
    return jax.shard_map(
        on_device,
        mesh=mesh,
        in_specs=placed,
        out_specs=(P("district", "sub", None), P("district", "sub", None), P()),
        check_vma=False,
    )
```

```python
import functools
import math

import jax
import jax.numpy as jnp
from jax import lax
from jax.experimental import pallas as pl
from jax.experimental.pallas import tpu as pltpu
from jax.sharding import PartitionSpec as P

REACH_SPAN = 16
LINK_COUNT = 4
RESERVOIRS = 16
OUTER_ITERS = 2
INNER_ITERS = 4
HALO = 2 * REACH_SPAN
LANES = 128

price_step = 0.3
reserve_step = 1.0

F32 = jnp.float32
BF16 = jnp.bfloat16
MESH = pl.DeviceIdType.MESH


def each(count, body):
    if count <= 8:
        for index in range(count):
            body(index)
    else:
        lax.fori_loop(0, count, lambda index, carry: (body(index), carry)[1], 0)


def mm(a, b):
    return jnp.dot(a, b, preferred_element_type=F32)


def contract(a, b, dim):
    return lax.dot_general(a, b, (((dim,), (dim,)), ((), ())), preferred_element_type=F32)


def fold(wide, half):
    tail = wide[:, LANES:]
    lane = lax.broadcasted_iota(jnp.int32, (half, LANES), 1)
    folded = jnp.where(lane < LANES // 2, tail[:half], pltpu.roll(tail[half:], LANES // 2, 1))
    return jnp.concatenate([wide[:, :LANES], folded], axis=0)


def unfold(folded, rows):
    tail = folded[rows:]
    return jnp.concatenate([tail, pltpu.roll(tail, LANES // 2, 1)], axis=0)


def unfolded(folded, rows):
    return jnp.concatenate([folded[:rows], unfold(folded, rows)], axis=1)


def response(powers):
    shift, summed = [], []
    for i in range(INNER_ITERS):
        chosen, added = 0.0, 0.0
        for j in range(i, INNER_ITERS):
            scale = price_step ** j
            chosen = chosen + scale * math.comb(INNER_ITERS - 1, i) * math.comb(INNER_ITERS - 1 - i, j - i) * powers[j]
            weight = sum(math.comb(k, i) * math.comb(k - i, j - i) for k in range(j, INNER_ITERS))
            added = added + price_step * scale * weight * powers[j + 1]
        shift.append(chosen)
        summed.append(added)
    return jnp.concatenate(shift, axis=0), jnp.concatenate(summed, axis=0)


def whole_wait(place_ref, start, count, send_sem, recv_sem, device):
    places = place_ref.at[pl.ds(start, count)]
    return pltpu.make_async_remote_copy(
        src_ref=places, dst_ref=places, send_sem=send_sem, recv_sem=recv_sem, device_id=device, device_id_type=MESH
    )


def target_of(index, me, count, width):
    place, turn = me // width, lax.rem(me, width)
    pairs = count // width
    if index >= count - width:
        return place * width + lax.rem(turn + 1 + index - (count - width), width)
    slot = index // width
    low = 1 - jnp.minimum(place // (pairs // 2), 1)
    climb = slot + jnp.minimum(jnp.maximum(slot - place + 1, 0), 1)
    fall = pairs - 1 - slot
    fall = fall - jnp.minimum(jnp.maximum(place - fall + 1, 0), 1)
    return (low * fall + (1 - low) * climb) * width + lax.rem(turn + 1 + index % width, width)


def chunks_of(unknowns):
    return 1 if unknowns % 128 == 0 else 1


def kernel(
    dual_scale, costs_hbm, near_hbm, owner_hbm, relayout_hbm, capacity_hbm, coupling_hbm, factor_hbm,
    plan_ref, prices_ref, duals_ref,
    costs_ref, near_ref, owner_ref, relayout_ref, capacity_ref, coupling, factor, tables, near, links, owners, wide_first, first, landed, gathered, base, state, flow, total, spread, inner, weight, answer, reply, replies,
    match_t, owned, onehot, select, near_links, factors_out, factors_in, chosen_out, chosen_in, prices_out, prices_in, duals, draws, arrived, returned, returning,
    local_sem, near_send, near_recv, flow_send, flow_recv, draw_send, draw_recv, reply_send, reply_recv, return_send, return_recv,
    factors_send, factors_recv, price_send, price_recv, dual_send, dual_recv,
):
    districts, rows, unknowns = costs_ref.shape
    interface = coupling.shape[1]
    horizon = capacity_ref.shape[1]
    group = relayout_ref.shape[1]
    sub_count = lax.axis_size("sub")
    district_count = lax.axis_size("district")
    me = lax.axis_index("sub")
    role = lax.rem(me, districts)
    team = me // districts * districts
    my_district = lax.axis_index("district")
    block = districts * rows
    window = block + 2 * HALO
    blocks = group // block
    half_count = sub_count // 2
    front = 1 - jnp.minimum(me // half_count, 1)

    def slot_of(source, place):
        far = jnp.minimum(place // half_count, 1)
        return lax.rem(source + far * half_count, sub_count)

    chunks = chunks_of(unknowns)
    chunk = unknowns // chunks
    small_loads = [
        pltpu.make_async_copy(source, target, local_sem.at[index])
        for index, (source, target) in enumerate(
            (
                (near_hbm, near_ref),
                (owner_hbm, owner_ref),
                (relayout_hbm, relayout_ref),
                (capacity_hbm, capacity_ref),
            )
        )
    ]
    costs_load = pltpu.make_async_copy(costs_hbm, costs_ref, local_sem.at[4])
    costs_load.start()
    loads = []
    for turn in range(districts):
        d = lax.rem(role + 1 + turn, districts)
        loads.append([])
        for part in range(chunks):
            at = pl.ds(part * chunk, chunk)
            loads[-1].append(pltpu.make_async_copy(factor_hbm.at[d, at], factor.at[d, at], local_sem.at[5 + turn * (chunks + 1) + part]))
        loads[-1].append(pltpu.make_async_copy(coupling_hbm.at[d], coupling.at[d], local_sem.at[5 + turn * (chunks + 1) + chunks]))
        for load in loads[-1]:
            load.start()
        if turn == 0:
            for load in small_loads:
                load.start()

    barrier = pltpu.get_barrier_semaphore()
    for step in range(1, sub_count):
        pl.semaphore_signal(
            barrier, inc=1, device_id={"sub": lax.rem(me + step, sub_count)}, device_id_type=MESH
        )
    for step in range(1, district_count):
        for other in range(districts):
            pl.semaphore_signal(
                barrier,
                inc=1,
                device_id={
                    "district": lax.rem(my_district + step, district_count),
                    "sub": team + lax.rem(role + other, districts),
                },
                device_id_type=MESH,
            )

    beside = {"sub": lax.rem(me + 1, sub_count)}
    near_all = whole_wait(near, 0, sub_count - 1, near_send.at[0], near_recv.at[0], beside)
    flow_all = whole_wait(landed, 0, sub_count - 1, flow_send.at[0], flow_recv.at[0], beside)
    flow_own = whole_wait(landed, 0, half_count - 1, flow_send.at[0], flow_recv.at[0], beside)
    flow_far = whole_wait(landed, 0, half_count, flow_send.at[0], flow_recv.at[1], beside)
    def send_to(index, source_ref, place_ref, send_sem, recv_sem):
        pltpu.make_async_remote_copy(
            src_ref=source_ref,
            dst_ref=place_ref,
            send_sem=send_sem,
            recv_sem=recv_sem,
            device_id={"sub": target_of(index, me, sub_count, districts)},
            device_id_type=MESH,
        ).start()

    def send_tables():
        pl.semaphore_wait(barrier, sub_count - 1 + (district_count - 1) * districts)
        for index in range(sub_count - 1):
            target = target_of(index, me, sub_count, districts)
            send_to(index, tables.at[lax.rem(target, districts)], near.at[me], near_send.at[0], near_recv.at[0])

    def send_flows(turn):
        for index in range(sub_count - 1):
            if index % districts == turn:
                target = target_of(index, me, sub_count, districts)
                send_to(index, first.at[lax.rem(target, districts)], landed.at[slot_of(me, target)], flow_send.at[0], flow_recv.at[1 if index < half_count else 0])

    def compute_first(turn):
        d = lax.rem(role + 1 + turn, districts)
        first_plan = jnp.zeros((rows, unknowns), F32)
        for part in range(chunks):
            loads[turn][part].wait()
            at = slice(part * chunk, (part + 1) * chunk)
            product = mm(costs_ref[d, :, at], factor[d, at, :])
            first_plan = product if part == 0 else first_plan + product
        loads[turn][chunks].wait()
        first_plan = -first_plan
        plan_ref[d] = first_plan
        wide_first[:, :interface] = contract(first_plan.astype(BF16), coupling[d], 1)
        first[d] = fold(wide_first[...], rows // 2).astype(BF16)

    costs_load.wait()
    for load in small_loads:
        load.wait()
    for d in range(districts):
        for k in range(LINK_COUNT):
            tables[d, k // 2 : k // 2 + 1, k % 2 * rows : (k % 2 + 1) * rows] = near_ref[d * LINK_COUNT + k : d * LINK_COUNT + k + 1, :]
        tables[d, LINK_COUNT // 2 : LINK_COUNT // 2 + 1, :rows] = owner_ref[d : d + 1, :]
    compute_first(0)
    send_tables()
    send_flows(0)
    for turn in range(1, districts):
        compute_first(turn)
        send_flows(turn)

    landed[slot_of(me, me)] = first[role]
    for d in range(districts):
        inner[d] = mm(coupling[d], factor[d]).astype(BF16)
        weight[d] = jnp.zeros_like(weight[d])
        weight[d, :, :interface] = (-contract(inner[d], coupling[d], 1)).astype(BF16)

    span = 2 * LANES
    pitch = span // INNER_ITERS
    row = lax.broadcasted_iota(jnp.int32, (pitch, 2 * LANES), 0)
    column = lax.broadcasted_iota(jnp.int32, (pitch, 2 * LANES), 1)
    powers = [[jnp.where((row == column) & (row < horizon), 1.0, 0.0)] for _ in range(districts)]
    for d in range(districts):
        powers[d].append(jnp.where(row < horizon, weight[d, :pitch, :].astype(F32), 0.0))
    for _ in range(INNER_ITERS - 1):
        for d in range(districts):
            last = powers[d][-1][:, :interface]
            high = last.astype(BF16)
            low = (last - high.astype(F32)).astype(BF16)
            both = mm(jnp.concatenate([high, low], axis=0), weight[d])
            powers[d].append(both[:pitch] + both[pitch:])
    replied = []
    for d in range(districts):
        chosen, added = response(powers[d])
        answer[:, 2 * d * span : (2 * d + 1) * span] = chosen.astype(BF16)
        answer[:, (2 * d + 1) * span : (2 * d + 2) * span] = added.astype(BF16)
        reply[d] = response(powers[d][1:] + powers[d][:1])[0][:, :LANES].T[:horizon].astype(BF16)

    partners = [
        (step, other)
        for step in range(district_count)
        for other in range(districts)
        if step or other
    ]

    def partner(step, other):
        return {
            "district": lax.rem(my_district + step, district_count),
            "sub": team + lax.rem(role + other, districts),
        }

    reply_copies = []
    for step in range(1, district_count):
        reply_copies.append(
            pltpu.make_async_remote_copy(
                src_ref=reply,
                dst_ref=replies.at[step],
                send_sem=reply_send.at[0],
                recv_sem=reply_recv.at[0],
                device_id={"district": lax.rem(my_district + step, district_count)},
                device_id_type=MESH,
            )
        )
        reply_copies[-1].start()

    moves = relayout_ref[pl.ds(role, 1), :]
    moves = jnp.where(front == 1, moves, jnp.concatenate([moves[:, group // 2 :], moves[:, : group // 2]], axis=1))
    team_rows = districts * rows
    pick = lax.broadcasted_iota(jnp.int32, (team_rows, group), 1) == (
        lax.broadcasted_iota(jnp.int32, (team_rows, group), 0) + team * rows - (1 - front) * (group // 2)
    )
    pick = jnp.where(pick, 1.0, 0.0).astype(BF16)

    kept = onehot.shape[0] == blocks

    def one_hot(b):
        place = lax.broadcasted_iota(jnp.int32, (block, group), 0) + b * block
        return jnp.where(place == moves, 1.0, 0.0).astype(BF16)

    def choose(b):
        chosen = one_hot(b)
        if kept:
            onehot[b] = chosen
        select[b] = contract(pick, chosen, 1).astype(BF16)

    each(blocks, choose)

    duals[...] = jnp.zeros_like(duals)
    duals[:, :horizon] = capacity_ref[...]
    flow[...] = jnp.zeros_like(flow)
    owned[...] = jnp.zeros_like(owned)
    links[...] = jnp.full_like(links, -window * 4)

    near[me] = tables[role]
    near_all.wait_recv()
    for source in range(sub_count):
        for k in range(LINK_COUNT):
            links[k : k + 1, HALO + source * rows : HALO + (source + 1) * rows] = near[source, k // 2 : k // 2 + 1, k % 2 * rows : (k % 2 + 1) * rows]
        owners[:, source * rows : (source + 1) * rows] = near[source, LINK_COUNT // 2 : LINK_COUNT // 2 + 1, :rows]
    own = owners[...]
    held = lax.broadcasted_iota(jnp.int32, (RESERVOIRS, group), 0)
    match_t[...] = jnp.where(held == own, 1.0, 0.0).astype(BF16)
    held = lax.broadcasted_iota(jnp.int32, (LANES, group), 0)
    hit = (lax.rem(held, RESERVOIRS) == own) & (held < INNER_ITERS * RESERVOIRS)
    owned[0, HALO : HALO + group, :] = jnp.where(hit, 1.0, 0.0).T.astype(BF16)

    def linked(start, width):
        column = lax.broadcasted_iota(jnp.int32, (width, width), 0)
        row = lax.broadcasted_iota(jnp.int32, (width, width), 1)
        table = jnp.where(column == row, 1.0, 0.0)
        for k in range(LINK_COUNT):
            link = links[k : k + 1, pl.ds(start, width)] - (start - HALO)
            table = table - jnp.where(column == link, 1.0 / LINK_COUNT, 0.0)
        return table.T.astype(BF16)

    def build(b):
        start = b * block if isinstance(b, int) else pl.multiple_of(b * block, block)
        table = linked(start, window)
        near_links[b] = table[HALO : HALO + block]
        spread[b] = mm(table[HALO : HALO + block], table).astype(BF16)

    each(blocks, build)
    my_links = near_links.at[team // districts]

    def at_block(b, extra=0, size=block):
        return pl.ds(b * block + extra if isinstance(b, int) else pl.multiple_of(b * block, block) + extra, size)

    lane = lax.broadcasted_iota(jnp.int32, (block, LANES), 1)

    team_window = pl.ds(pl.multiple_of(team * rows, team_rows), window)
    side = lax.broadcasted_iota(jnp.int32, (RESERVOIRS // 2, LANES), 1)

    def halved(values):
        return jnp.where(side < LANES // 2, values[: RESERVOIRS // 2], pltpu.roll(values[RESERVOIRS // 2 :], LANES // 2, 1))

    def whole(values):
        return jnp.concatenate([values, pltpu.roll(values, LANES // 2, 1)], axis=0)

    capacity = halved(duals[...])

    def to_team(source_ref, place_ref, send_sem, recv_sem):
        copies = []
        for other in range(1, districts):
            target = lax.rem(role + other, districts)
            copies.append(
                pltpu.make_async_remote_copy(
                    src_ref=source_ref.at[target],
                    dst_ref=place_ref.at[role],
                    send_sem=send_sem.at[other - 1],
                    recv_sem=recv_sem.at[other - 1],
                    device_id={"sub": team + target},
                    device_id_type=MESH,
                )
            )
            copies[-1].start()
        place_ref[role] = source_ref[role]
        return copies

    def chosen_rows(values):
        chosen = mm(select[0], values(0))
        for b in range(1, blocks):
            chosen = chosen + mm(select[b], values(b))
        return chosen

    for turn in range(1, INNER_ITERS):
        now, later = owned.at[(turn + 1) % 2], owned.at[turn % 2]

        def lengthen(b, turn=turn, now=now, later=later):
            held = now[at_block(b, HALO), :].astype(F32)
            out = mm(spread[b], now[at_block(b, 0, window), :]) - held
            later[at_block(b, HALO), :] = jnp.where(lane < turn * RESERVOIRS, held, out).astype(BF16)

        each(blocks, lengthen)
    owned_all = owned.at[(INNER_ITERS - 1) % 2]

    picked = chosen_rows(lambda b: owned_all[at_block(b, HALO), :])
    local = mm(my_links[...], owned_all[team_window, :])
    factors = jnp.where(lane < LANES // 2, picked, pltpu.roll(local, LANES // 2, 1))
    factors_out[...] = factors.reshape(districts, rows, LANES).astype(BF16)
    returned[...] = halved(mm(match_t[...], owned_all[HALO : HALO + group, :])).astype(BF16)
    factor_copies = to_team(factors_out, factors_in, factors_send, factors_recv)
    return_copies = []
    for index, (step, other) in enumerate(partners):
        return_copies.append(
            pltpu.make_async_remote_copy(
                src_ref=returned,
                dst_ref=returning.at[index],
                send_sem=return_send.at[0],
                recv_sem=return_recv.at[0],
                device_id=partner(step, other),
                device_id_type=MESH,
            )
        )
        return_copies[-1].start()


    spare = lax.broadcasted_iota(jnp.int32, (rows, LANES), 1) < interface - LANES

    def spread_out(source):
        at = pl.ds(source * rows, rows)
        gathered[at, :LANES] = landed[source, :rows, :]
        tail = unfold(landed[source].astype(F32), rows)
        gathered[at, LANES:] = jnp.where(spare, tail, 0.0).astype(BF16)

    middle = group // 2

    def permute(b):
        chosen = onehot[b] if kept else one_hot(b)
        base[at_block(b), :] = mm(chosen[:, :middle], gathered[:middle, :])

    def permute_far(b):
        chosen = onehot[b] if kept else one_hot(b)
        moved = base[at_block(b), :] + mm(chosen[:, middle:], gathered[middle:, :])
        base[at_block(b), :] = moved
        flow[at_block(b, HALO), :] = moved.astype(BF16)

    flow_own.wait_recv()
    each(half_count, spread_out)
    each(blocks, permute)
    flow_far.wait_recv()
    each(half_count, lambda source: spread_out(source + half_count))
    each(blocks, permute_far)

    total[...] = flow[team_window, :].astype(F32)

    def forward():
        def one(b):
            price = state[at_block(b), :interface].astype(BF16)
            flow[at_block(b, HALO), :] = (base[at_block(b), :] + mm(price, weight[role])).astype(BF16)

        each(blocks, one)
        total[...] += flow[team_window, :].astype(F32)

    def backward(fresh=False):
        def one(b):
            out = mm(spread[b], flow[at_block(b, 0, window), :])
            gain = price_step * out
            state[at_block(b), :] = gain if fresh else state[at_block(b), :] + gain

        each(blocks, one)

    def start_draws(outer):
        copies = []
        for index, (step, other) in enumerate(partners):
            copies.append(
                pltpu.make_async_remote_copy(
                    src_ref=draws.at[outer],
                    dst_ref=arrived.at[outer, index],
                    send_sem=draw_send.at[outer],
                    recv_sem=draw_recv.at[outer],
                    device_id=partner(step, other),
                    device_id_type=MESH,
                )
            )
            copies[-1].start()
        return copies

    def take_draws(outer, copies):
        drawn = draws[outer]
        whole_wait(arrived.at[outer], 0, len(partners), draw_send.at[outer], draw_recv.at[outer], partner(*partners[-1])).wait()
        for index in range(len(partners)):
            drawn = drawn + arrived[outer, index]
        return drawn - capacity

    backward(fresh=True)
    for step in range(1, INNER_ITERS - 1):
        forward()
        backward()
    forward()
    drawn = mm(match_t[...], flow[HALO : HALO + group, :])
    draws[0] = halved(drawn[:, :LANES])
    copies = start_draws(0)
    for step in range(INNER_ITERS - 1):
        backward()
        forward()
    backward()
    forward()
    drawn = mm(match_t[...], flow[HALO : HALO + group, :])
    draws[1] = halved(drawn[:, :LANES])
    chosen = chosen_rows(lambda b: state[at_block(b), :].astype(BF16))
    late_copies = start_draws(1)
    high = total[...].astype(BF16)
    low = (total[...] - high.astype(F32)).astype(BF16)
    for d in range(districts):
        chosen_out[d] = fold(chosen[d * rows : (d + 1) * rows], rows // 2).astype(BF16)
    price_copies = to_team(chosen_out, chosen_in, price_send, price_recv)
    prices = price_step * (mm(my_links[...], high) + mm(my_links[...], low))
    for d in range(districts):
        prices_out[d] = fold(prices[d * rows : (d + 1) * rows], rows // 2).astype(BF16)
    dual_copies = to_team(prices_out, prices_in, dual_send, dual_recv)

    for copy in factor_copies:
        copy.wait()
    across = partner(*partners[-1])
    whole_wait(returning, 0, len(partners), return_send.at[0], return_recv.at[0], across).wait()
    whole_wait(replies, 1, district_count - 1, reply_send.at[0], reply_recv.at[0], across).wait()
    heard = [whole(returned[...].astype(F32))] + [whole(returning[index].astype(F32)) for index in range(len(partners))]
    heard = jnp.concatenate(heard, axis=0)[:, : LANES // 2].astype(BF16)

    drawn = take_draws(0, copies)
    moved = whole(jnp.where(lax.rem(side, LANES // 2) < horizon, drawn * dual_scale, 0.0))
    lanes = lax.broadcasted_iota(jnp.int32, moved.shape, 1)
    moved = jnp.where(lanes < horizon, moved, 0.0)
    half = pltpu.roll(moved, pitch, 1)
    none = jnp.zeros_like(moved)
    steps = jnp.concatenate(
        [
            jnp.concatenate([moved, none], axis=1),
            jnp.concatenate([half, none], axis=1),
            jnp.concatenate([none, moved], axis=1),
            jnp.concatenate([none, half], axis=1),
        ],
        axis=0,
    ).astype(BF16)
    turned = mm(steps, answer[...]).astype(BF16)
    returns = mm(heard, steps).astype(BF16)
    changes = []
    for d in range(districts):
        fit = factors_in[d]
        changes.append(
            (
                mm(fit[:, : LANES // 2], turned[:, 2 * d * span : (2 * d + 1) * span])[:, :interface],
                mm(fit[:, LANES // 2 :], turned[:, (2 * d + 1) * span : (2 * d + 2) * span])[:, :interface],
            )
        )
    late = contract(returns[:RESERVOIRS], reply[role], 1)
    for index, (step, other) in enumerate(partners):
        at = slice((index + 1) * RESERVOIRS, (index + 2) * RESERVOIRS)
        source = lax.rem(role + districts - other, districts)
        late = late + contract(returns[at], replies[step, source] if step else reply[source], 1)
    for copy in price_copies:
        copy.wait()
    for d in range(districts):
        price = unfolded(chosen_in[d].astype(F32), rows)[:, :interface] + changes[d][0]
        plan_ref[d] = plan_ref[d] - mm(price.astype(BF16), inner[d])
    for copy in dual_copies:
        copy.wait()
    for d in range(districts):
        prices_ref[d] = unfolded(prices_in[d].astype(F32), rows)[:, :interface] + changes[d][1]
    drawn = whole(take_draws(1, late_copies))
    duals_ref[...] = moved[:, :horizon] + (drawn[:, :horizon] + late) * dual_scale
    near_all.wait_send()
    flow_all.wait_send()


def handover(plan_ref, prices_ref, duals_ref, plan_out, prices_out, duals_out, sem):
    copies = [
        pltpu.make_async_copy(source, target, sem.at[index])
        for index, (source, target) in enumerate(
            ((plan_ref, plan_out), (prices_ref, prices_out), (duals_ref, duals_out))
        )
    ]
    for copy in copies:
        copy.start()
    for copy in copies:
        copy.wait()


def on_device(cost_terms, neighbours, relayout, ownership, capacity, coupling, solve_factor):
    districts, rows, unknowns = cost_terms.shape
    interface = coupling.shape[2]
    group = relayout.shape[1]
    sub_count = lax.axis_size("sub")
    district_count = lax.axis_size("district")
    load_count = districts * district_count * group // (2 * RESERVOIRS)
    dual_scale = reserve_step / math.sqrt(load_count)
    near = neighbours.transpose(0, 2, 1).reshape(districts * LINK_COUNT, rows)
    coupling = coupling.transpose(0, 2, 1)
    block = districts * rows
    blocks = group // block
    window = block + 2 * HALO
    vmem = pl.BlockSpec(memory_space=pltpu.VMEM)
    hbm = pl.BlockSpec(memory_space=pl.ANY)
    dma = pltpu.SemaphoreType.DMA
    results = pl.pallas_call(
        functools.partial(kernel, dual_scale),
        name="districts",
        out_shape=(
            jax.ShapeDtypeStruct((districts, rows, unknowns), F32),
            jax.ShapeDtypeStruct((districts, rows, interface), F32),
            jax.ShapeDtypeStruct(capacity.shape, F32),
        ),
        in_specs=[pl.BlockSpec(memory_space=pltpu.HBM)] * 7,
        out_specs=(vmem, vmem, vmem),
        scratch_shapes=[
            pltpu.VMEM(cost_terms.shape, BF16),
            pltpu.VMEM(near.shape, jnp.int32),
            pltpu.VMEM(ownership.shape, jnp.int32),
            pltpu.VMEM(relayout.shape, jnp.int32),
            pltpu.VMEM(capacity.shape, F32),
            pltpu.VMEM(coupling.shape, BF16),
            pltpu.VMEM(solve_factor.shape, BF16),
            pltpu.VMEM((districts, LINK_COUNT, LANES), jnp.int32),
            pltpu.VMEM((sub_count, LINK_COUNT, LANES), jnp.int32),
            pltpu.VMEM((LINK_COUNT, group + 2 * HALO), jnp.int32),
            pltpu.VMEM((1, group), jnp.int32),
            pltpu.VMEM((rows, 2 * LANES), F32),
            pltpu.VMEM((districts, rows + rows // 2, LANES), BF16),
            pltpu.VMEM((sub_count, rows + rows // 2, LANES), BF16),
            pltpu.VMEM((group, 2 * LANES), BF16),
            pltpu.VMEM((group, 2 * LANES), F32),
            pltpu.VMEM((group, 2 * LANES), F32),
            pltpu.VMEM((group + 2 * HALO, 2 * LANES), BF16),
            pltpu.VMEM((window, 2 * LANES), F32),
            pltpu.VMEM((blocks, block, window), BF16),
            pltpu.VMEM((districts, interface, unknowns), BF16),
            pltpu.VMEM((districts, interface, 2 * LANES), BF16),
            pltpu.VMEM((2 * LANES, 4 * LANES * districts), BF16),
            pltpu.VMEM((districts, capacity.shape[1], 2 * LANES), BF16),
            pltpu.VMEM((district_count, districts, capacity.shape[1], 2 * LANES), BF16),
            pltpu.VMEM((RESERVOIRS, group), BF16),
            pltpu.VMEM((2, group + 2 * HALO, LANES), BF16),
            pltpu.VMEM((blocks if group <= 1024 else 1, block, group), BF16),
            pltpu.VMEM((blocks, block, block), BF16),
            pltpu.VMEM((blocks, block, window), BF16),
            pltpu.VMEM((districts, rows, LANES), BF16),
            pltpu.VMEM((districts, rows, LANES), BF16),
            pltpu.VMEM((districts, rows + rows // 2, LANES), BF16),
            pltpu.VMEM((districts, rows + rows // 2, LANES), BF16),
            pltpu.VMEM((districts, rows + rows // 2, LANES), BF16),
            pltpu.VMEM((districts, rows + rows // 2, LANES), BF16),
            pltpu.VMEM((RESERVOIRS, LANES), F32),
            pltpu.VMEM((OUTER_ITERS, RESERVOIRS // 2, LANES), F32),
            pltpu.VMEM((OUTER_ITERS, district_count * districts, RESERVOIRS // 2, LANES), F32),
            pltpu.VMEM((RESERVOIRS // 2, LANES), BF16),
            pltpu.VMEM((district_count * districts, RESERVOIRS // 2, LANES), BF16),
            dma((districts * (chunks_of(unknowns) + 1) + 5,)),
            dma((1,)),
            dma((1,)),
            dma((1,)),
            dma((2,)),
            dma((OUTER_ITERS,)),
            dma((OUTER_ITERS,)),
            dma((1,)),
            dma((1,)),
            dma((1,)),
            dma((1,)),
            dma((districts - 1,)),
            dma((districts - 1,)),
            dma((districts - 1,)),
            dma((districts - 1,)),
            dma((districts - 1,)),
            dma((districts - 1,)),
        ],
        compiler_params=pltpu.CompilerParams(
            collective_id=0, has_side_effects=True, vmem_limit_bytes=(20 if group <= 1024 else 60) * 1024 * 1024
        ),
    )(*[pltpu.with_memory_space_constraint(value, pltpu.HBM) for value in (cost_terms, near, ownership, relayout, capacity, coupling, solve_factor)])
    return pl.pallas_call(
        handover,
        name="handover",
        out_shape=tuple(jax.ShapeDtypeStruct(value.shape, value.dtype) for value in results),
        in_specs=[hbm] * 3,
        out_specs=(hbm,) * 3,
        scratch_shapes=[dma((3,))],
        compiler_params=pltpu.CompilerParams(vmem_limit_bytes=4 * 1024 * 1024),
    )(*results)


def solution(mesh):
    placed = (
        P("district", "sub", None),
        P("district", "sub", None),
        P("district", None),
        P("district", "sub"),
        P(),
        P("district", None, None),
        P("district", None, None),
    )
    return jax.shard_map(
        on_device,
        mesh=mesh,
        in_specs=placed,
        out_specs=(P("district", "sub", None), P("district", "sub", None), P()),
        check_vma=False,
    )
```
